16 devices in a mesh: dp: 2 (over y, z), cp: 8 (over x, core).
Axes of the slice: x: 4, y: 2, z: 1, core: 2. Of those that a mesh axis runs over, the one named last changes fastest.
The devices are a block of a 4x4x8 slice.
Arguments:
- query: bfloat16 [8, 256, 32, 128], P('dp', 'cp'), parts along dimension 0
- key: bfloat16 [8, 256, 128], P('dp', 'cp'), parts along dimension 0
- value: bfloat16 [8, 256, 128], P('dp', 'cp'), parts along dimension 0
- positions: int32 [512], P(('dp', 'cp')), parts along dimension 0
- grad_out: bfloat16 [8, 256, 32, 128], P('dp', 'cp'), parts along dimension 0
Outputs:
- output 1: bfloat16 [8, 256, 32, 128], P('dp', 'cp'), parts along dimension 0
- output 2: bfloat16 [8, 256, 32, 128], P('dp', 'cp'), parts along dimension 0
- output 3: bfloat16 [8, 256, 128], P('dp', 'cp'), parts along dimension 0
- output 4: bfloat16 [8, 256, 128], P('dp', 'cp'), parts along dimension 0
There are 2 independent parts. The reference program is written for one: setup_inputs(seed, part) draws one part's arguments, and reference() takes and returns one part's arrays. A program takes and returns all parts, laid end to end along the dimension named above; each array names one.
All inputs are finite; a program needn't handle non-finite values.
Results may differ from the reference program's by a relative error of at most 0.00834231.
Values are sent between devices in bfloat16 or wider.
A program may use at most 768 MiB of HBM per device.

```python
import jax
import jax.numpy as jnp
from jax import lax

BATCH = 4
SEQ = 256
HEADS = 32
HEAD = 128
QROWS = 8
ROPE_BASE = 10000


def setup_inputs(seed: int = 0, part: int = 0) -> dict:
    part_key = jax.random.fold_in(jax.random.key(seed), part)
    rng_keys = jax.random.split(part_key, 6)
    query = jax.random.normal(rng_keys[0], (BATCH, SEQ, HEADS, HEAD), jnp.float32)
    key = jax.random.normal(rng_keys[1], (BATCH, SEQ, HEAD), jnp.float32)
    value = jax.random.normal(rng_keys[2], (BATCH, SEQ, HEAD), jnp.float32)
    start = jax.random.randint(rng_keys[3], (), 0, 256)
    increments = jax.random.randint(rng_keys[4], (SEQ,), 0, 2)
    positions = (start + jnp.cumsum(increments)).astype(jnp.int32)
    grad_out = jax.random.normal(rng_keys[5], (BATCH, SEQ, HEADS, HEAD), jnp.float32)
    return {'query': query.astype(jnp.bfloat16), 'key': key.astype(jnp.bfloat16), 'value': value.astype(jnp.bfloat16), 'positions': positions, 'grad_out': grad_out.astype(jnp.bfloat16)}


def rope_tables(positions):
    half_dim = HEAD // 2
    inv_freq = jnp.power(jnp.float32(ROPE_BASE), -2.0 * jnp.arange(half_dim, dtype=jnp.float32) / HEAD)
    angles = positions.astype(jnp.float32)[..., None] * inv_freq
    angles = jnp.concatenate([angles, angles], axis=-1)
    return jnp.cos(angles), jnp.sin(angles)


def rotate(values, cos_tab, sin_tab):
    half_dim = values.shape[-1] // 2
    turned = jnp.concatenate([-values[..., half_dim:], values[..., :half_dim]], axis=-1)
    return values * cos_tab + turned * sin_tab


def reference(query, key, value, positions, grad_out):
    cos_tab, sin_tab = rope_tables(positions)
    cos_q = cos_tab[None, :, None, :]
    sin_q = sin_tab[None, :, None, :]
    query_rot = rotate(query.astype(jnp.float32), cos_q, sin_q).astype(jnp.bfloat16)
    key_rot = rotate(key.astype(jnp.float32), cos_tab[None], sin_tab[None]).astype(jnp.bfloat16)
    scale = HEAD ** -0.5
    key_f = key_rot.astype(jnp.float32)
    value_f = value.astype(jnp.float32)
    key_idx = jnp.arange(SEQ)
    block_count = SEQ // QROWS
    query_blocks = query_rot.reshape(BATCH, block_count, QROWS, HEADS, HEAD).transpose(1, 0, 2, 3, 4)
    grad_blocks = grad_out.reshape(BATCH, block_count, QROWS, HEADS, HEAD).transpose(1, 0, 2, 3, 4)

    def one_block(carry, block):
        dkey_acc, dvalue_acc = carry
        query_blk, grad_blk, block_idx = block
        query_f = query_blk.astype(jnp.float32)
        grad_f = grad_blk.astype(jnp.float32)
        query_idx = block_idx * QROWS + jnp.arange(QROWS)
        causal_mask = (key_idx[None, :] <= query_idx[:, None])[None, :, None, :]
        scores = jnp.where(causal_mask, jnp.einsum('bqhd,bkd->bqhk', query_f, key_f) * scale, -jnp.inf)
        row_max = jnp.max(scores, axis=-1, keepdims=True)
        weights = jnp.exp(scores - row_max)
        row_sum = jnp.sum(weights, axis=-1, keepdims=True)
        attn_f = jnp.einsum('bqhk,bkd->bqhd', weights.astype(jnp.bfloat16).astype(jnp.float32), value_f) / row_sum
        attn_blk = attn_f.astype(jnp.bfloat16)
        probs_f = jnp.exp(scores - (row_max + jnp.log(row_sum)))
        delta = jnp.sum(grad_f * attn_blk.astype(jnp.float32), axis=-1, keepdims=True)
        dprobs = jnp.einsum('bqhd,bkd->bqhk', grad_f, value_f)
        dscore = (probs_f * (dprobs - delta)).astype(jnp.bfloat16).astype(jnp.float32)
        dquery_blk = jnp.einsum('bqhk,bkd->bqhd', dscore, key_f) * scale
        dkey_acc = dkey_acc + jnp.einsum('bqhk,bqhd->bkd', dscore, query_f) * scale
        dvalue_acc = dvalue_acc + jnp.einsum('bqhk,bqhd->bkd', probs_f.astype(jnp.bfloat16).astype(jnp.float32), grad_f)
        return (dkey_acc, dvalue_acc), (attn_blk, dquery_blk)

    zero_kv = jnp.zeros((BATCH, SEQ, HEAD), jnp.float32)
    sums, outs = lax.scan(one_block, (zero_kv, zero_kv), (query_blocks, grad_blocks, jnp.arange(block_count)))
    attn_out = outs[0].transpose(1, 0, 2, 3, 4).reshape(BATCH, SEQ, HEADS, HEAD)
    dquery_rot = outs[1].transpose(1, 0, 2, 3, 4).reshape(BATCH, SEQ, HEADS, HEAD)
    grad_query = rotate(dquery_rot, cos_q, -sin_q).astype(jnp.bfloat16)
    grad_key = rotate(sums[0], cos_tab[None], -sin_tab[None]).astype(jnp.bfloat16)
    grad_value = sums[1].astype(jnp.bfloat16)
    return (attn_out, grad_query, grad_key, grad_value)
```

```python
import functools

import jax
import jax.numpy as jnp
import numpy as np
from jax import lax
from jax.experimental import pallas as pl
from jax.experimental.pallas import tpu as pltpu
from jax.sharding import PartitionSpec as P

ROPE_BASE = 10000
CORES = 2
LOG2E = 1.4426950408889634
F32 = jnp.float32
BF16 = jnp.bfloat16
ROWS = 512


def dot_nn(a, b):
    return jnp.dot(a, b, preferred_element_type=F32)


def dot_nt(a, b):
    return lax.dot_general(a, b, (((1,), (1,)), ((), ())), preferred_element_type=F32)


def attend_kernel(cp, blk, q_hbm, g_hbm, k_hbm, v_hbm, pos_hbm, freq_hbm,
                  o_ref, dq_ref, rbuf, tabs_out,
                  k_ref, v_ref, pos_ref, freq_ref, qb, gb, rq, tabs, kvown, kvb, p_t, ds_t, part, osib, dqsib,
                  first_sem, loc_sem, qg_send, qg_recv, tab_send, tab_recv, kv_send, kv_recv,
                  r_send, r_recv, od_send, od_recv):
    chips = cp // CORES
    seqs = q_hbm.shape[0]
    mine = seqs // CORES
    rows, head = q_hbm.shape[1], q_hbm.shape[2]
    heads = rows // blk
    half_dim = head // 2
    keys = cp * blk
    scale = head ** -0.5
    me = lax.axis_index("cp")
    chip = lax.div(me, CORES)
    core = lax.rem(me, CORES)
    sib = chip * CORES + 1 - core

    def remote(src, dst, ssem, rsem, dev):
        return pltpu.make_async_remote_copy(src_ref=src, dst_ref=dst, send_sem=ssem, recv_sem=rsem,
                                            device_id={"cp": dev}, device_id_type=pl.DeviceIdType.MESH)

    first = [pltpu.make_async_copy(src, dst, first_sem.at[n]) for n, (src, dst) in enumerate(
        ((pos_hbm, pos_ref), (freq_hbm, freq_ref), (k_hbm, k_ref), (v_hbm, v_ref)))]
    for c in first:
        c.start()
    local = []
    for s in range(mine):
        local.append(pltpu.make_async_copy(q_hbm.at[core * mine + s], qb.at[s, 0], loc_sem.at[0, s]))
        local.append(pltpu.make_async_copy(g_hbm.at[core * mine + s], gb.at[s, 0], loc_sem.at[1, s]))
    for c in local:
        c.start()

    kvb[...] = jnp.zeros_like(kvb)
    rbuf[...] = jnp.zeros_like(rbuf)

    barrier = pltpu.get_barrier_semaphore()
    for d in range(1, cp):
        pl.semaphore_signal(barrier, inc=1, device_id={"cp": lax.rem(me + d, cp)},
                            device_id_type=pl.DeviceIdType.MESH)

    for c in first:
        c.wait()
    pos_row = jnp.broadcast_to(pos_ref[...].astype(F32), (blk, blk))
    ident = lax.broadcasted_iota(jnp.int32, (blk, blk), 0) == lax.broadcasted_iota(jnp.int32, (blk, blk), 1)
    pos_col = jnp.sum(jnp.where(ident, pos_row, 0.0), axis=1, keepdims=True)
    ang = pos_col * freq_ref[...]
    cos_t = jnp.cos(ang)
    lane = lax.broadcasted_iota(jnp.int32, (blk, head), 1)
    sin_t = jnp.where(lane < half_dim, -jnp.sin(ang), jnp.sin(ang))
    tabs[0, 0] = cos_t
    tabs[0, 1] = sin_t
    tabs_out[0] = cos_t
    tabs_out[1] = sin_t
    for b in range(seqs):
        kf = k_ref[b].astype(F32)
        kvown[b, 0] = (kf * cos_t + pltpu.roll(kf, half_dim, 1) * sin_t).astype(BF16)
        kvown[b, 1] = v_ref[b]

    pl.semaphore_wait(barrier, cp - 1)

    tab_copy = remote(tabs.at[0], tabs.at[1], tab_send, tab_recv, sib)
    tab_copy.start()

    def kv_copy(s, c2, k2):
        return remote(kvown.at[k2 * mine + s], kvb.at[s, me], kv_send.at[s, c2, k2], kv_recv.at[s, me],
                      c2 * CORES + k2)

    def kv_sib(s):
        return remote(kvown.at[(1 - core) * mine + s], kvb.at[s, me], kv_send.at[s, chip, 1 - core],
                      kv_recv.at[s, me], sib)

    def qg_copies(s):
        return (remote(q_hbm.at[(1 - core) * mine + s], qb.at[s, 1], qg_send.at[0, s], qg_recv.at[0, s], sib),
                remote(g_hbm.at[(1 - core) * mine + s], gb.at[s, 1], qg_send.at[1, s], qg_recv.at[1, s], sib))

    for s in range(mine):
        for c2 in range(chips):
            for k2 in range(CORES):
                @pl.when(c2 > chip)
                def _():
                    kv_copy(s, c2, k2).start()
        kv_sib(s).start()
        for c in qg_copies(s):
            c.start()
    for s in range(mine):
        kvb[s, me] = kvown[core * mine + s]

    def rope_q(s, h):
        x = qb[s, h].astype(F32)
        cos_q = jnp.broadcast_to(tabs[h, 0][:, None, :], (blk, heads, head)).reshape(rows, head)
        sin_q = jnp.broadcast_to(tabs[h, 1][:, None, :], (blk, heads, head)).reshape(rows, head)
        rq[s, h * rows:(h + 1) * rows, :] = (x * cos_q + pltpu.roll(x, half_dim, 1) * sin_q).astype(BF16)

    for c in local:
        c.wait()
    for s in range(mine):
        rope_q(s, 0)
    tab_copy.wait_recv()
    for s in range(mine):
        for c in qg_copies(s):
            c.wait_recv()
        rope_q(s, 1)

    def part_copy(s, x, c2, k2):
        return remote(part.at[s, c2 * CORES + k2, x], rbuf.at[chip, core * mine + s, x],
                      r_send.at[s, x, c2, k2], r_recv.at[chip, core * mine + s, x], c2 * CORES + k2)

    def part_sib(s, x):
        return remote(part.at[s, sib, x], rbuf.at[chip, core * mine + s, x],
                      r_send.at[s, x, chip, 1 - core], r_recv.at[chip, core * mine + s, x], sib)

    def send_part(s, x, val):
        part[s, :, x] = val.reshape(cp, blk, head)
        for c2 in range(chips):
            for k2 in range(CORES):
                @pl.when(c2 < chip)
                def _():
                    part_copy(s, x, c2, k2).start()
        part_sib(s, x).start()
        rbuf[chip, core * mine + s, x] = part[s, me, x]

    def out_copy(which, s):
        src, dst = ((osib, o_ref), (dqsib, dq_ref))[which]
        return remote(src.at[s], dst.at[core * mine + s], od_send.at[which, s], od_recv.at[which, s], sib)

    key_idx = lax.broadcasted_iota(jnp.int32, (keys, ROWS), 0)
    row_tok = lax.div(lax.broadcasted_iota(jnp.int32, (1, ROWS), 1), heads)

    for s in range(mine):
        for j in range(cp):
            @pl.when(jnp.logical_and(j < (chip + 1) * CORES, j != me))
            def _():
                pltpu.make_async_remote_copy(src_ref=kvown.at[s], dst_ref=kvb.at[s, j], send_sem=kv_send.at[s, 0, 0],
                                             recv_sem=kv_recv.at[s, j], device_id={"cp": sib},
                                             device_id_type=pl.DeviceIdType.MESH).wait_recv()
        kk = kvb[s, :, 0].reshape(keys, head)
        vv = kvb[s, :, 1].reshape(keys, head)
        v_t = vv.T
        for h in (1, 0):
            base = jnp.where(h == 0, me, sib) * blk
            for r in range(0, rows, ROWS):
                row0 = h * rows + r
                g = gb[s, h, r:r + ROWS, :]
                x = dot_nt(kk, rq[s, row0:row0 + ROWS, :])
                tok = row_tok + (base + r // heads)
                x = jnp.where(key_idx <= tok, x, -jnp.inf)
                mx = jnp.max(x, axis=0, keepdims=True)
                w = jnp.exp2((x - mx) * (scale * LOG2E))
                inv_l = 1.0 / jnp.sum(w, axis=0, keepdims=True)
                o_t = (dot_nn(v_t, w.astype(BF16)) * inv_l).astype(BF16)
                p = w * inv_l
                p_t[s, :, row0:row0 + ROWS] = p.astype(BF16)
                delta = jnp.sum(g.T.astype(F32) * o_t.astype(F32), axis=0, keepdims=True)
                dp = dot_nt(vv, g)
                ds_t[s, :, row0:row0 + ROWS] = (p * (dp - delta)).astype(BF16)
                if h == 0:
                    o_ref[core * mine + s, r:r + ROWS, :] = o_t.T
                else:
                    osib[s, r:r + ROWS, :] = o_t.T
            if h == 1:
                out_copy(0, s).start()
        send_part(s, 1, dot_nn(p_t[s], gb[s].reshape(CORES * rows, head)))
        send_part(s, 0, dot_nn(ds_t[s], rq[s]))

    for s in range(mine):
        k_t = kvb[s, :, 0].reshape(keys, head).T
        for h in (1, 0):
            for r in range(0, rows, ROWS):
                row0 = h * rows + r
                dqr = dot_nn(k_t, ds_t[s, :, row0:row0 + ROWS]).T * scale
                toks = ROWS // heads
                t0 = r // heads
                cos_q = jnp.broadcast_to(tabs[h, 0, t0:t0 + toks][:, None, :], (toks, heads, head)).reshape(ROWS, head)
                sin_q = jnp.broadcast_to(tabs[h, 1, t0:t0 + toks][:, None, :], (toks, heads, head)).reshape(ROWS, head)
                dq = (dqr * cos_q - pltpu.roll(dqr, half_dim, 1) * sin_q).astype(BF16)
                if h == 0:
                    dq_ref[core * mine + s, r:r + ROWS, :] = dq
                else:
                    dqsib[s, r:r + ROWS, :] = dq
            if h == 1:
                out_copy(1, s).start()

    for s in range(mine):
        for x in range(2):
            out_copy(x, s).wait()
            part_sib(s, x).wait_send()
            remote(part.at[s, sib, x], rbuf.at[chip, (1 - core) * mine + s, x], r_send.at[s, x, chip, 1 - core],
                   r_recv.at[chip, (1 - core) * mine + s, x], sib).wait_recv()
            for c2 in range(chips):
                for k2 in range(CORES):
                    @pl.when(c2 < chip)
                    def _():
                        part_copy(s, x, c2, k2).wait_send()

                    @pl.when(c2 > chip)
                    def _():
                        pltpu.make_async_remote_copy(
                            src_ref=part.at[s, 0, x], dst_ref=rbuf.at[c2, k2 * mine + s, x],
                            send_sem=r_send.at[s, x, 0, 0], recv_sem=r_recv.at[c2, k2 * mine + s, x],
                            device_id={"cp": sib}, device_id_type=pl.DeviceIdType.MESH).wait_recv()
        kv_sib(s).wait_send()
        for c in qg_copies(s):
            c.wait_send()
        for c2 in range(chips):
            for k2 in range(CORES):
                @pl.when(c2 > chip)
                def _():
                    kv_copy(s, c2, k2).wait_send()
    tab_copy.wait_send()


def finish_kernel(o_in, dq_in, rbuf, tabs, o_hbm, dq_hbm, dk_ref, dv_ref, sem):
    copies = [pltpu.make_async_copy(o_in, o_hbm, sem.at[0]), pltpu.make_async_copy(dq_in, dq_hbm, sem.at[1])]
    for c in copies:
        c.start()
    head = tabs.shape[-1]
    scale = head ** -0.5
    cos_t, sin_t = tabs[0], tabs[1]
    for b in range(dk_ref.shape[0]):
        dk = rbuf[0, b, 0]
        dv = rbuf[0, b, 1]
        for c in range(1, rbuf.shape[0]):
            dk = dk + rbuf[c, b, 0]
            dv = dv + rbuf[c, b, 1]
        dk = dk * scale
        dk_ref[b] = (dk * cos_t - pltpu.roll(dk, head // 2, 1) * sin_t).astype(BF16)
        dv_ref[b] = dv.astype(BF16)
    for c in copies:
        c.wait()


def solution(mesh):
    cp = mesh.shape["cp"]
    query_spec = P("dp", "cp", None, None)
    kv_spec = P("dp", "cp", None)
    pos_spec = P(("dp", "cp"))

    def per_device(query, key, value, positions, grad_out):
        seqs, blk, heads, head = query.shape
        rows = blk * heads
        chips = cp // CORES
        mine = seqs // CORES
        keys = cp * blk
        freq = np.power(float(ROPE_BASE), -2.0 * np.arange(head // 2) / head)
        freq = jnp.asarray(np.concatenate([freq, freq])[None, :].astype(np.float32))
        vmem = pl.BlockSpec(memory_space=pltpu.VMEM)
        hbm = pl.BlockSpec(memory_space=pltpu.HBM)
        dma = pltpu.SemaphoreType.DMA
        big = jax.ShapeDtypeStruct((seqs, rows, head), BF16)
        small = jax.ShapeDtypeStruct((seqs, blk, head), BF16)
        o_mid, dq_mid, rbuf, tabs = pl.pallas_call(
            functools.partial(attend_kernel, cp, blk),
            out_shape=[big, big, jax.ShapeDtypeStruct((chips, seqs, 2, blk, head), F32),
                       jax.ShapeDtypeStruct((2, blk, head), F32)],
            in_specs=[hbm] * 6,
            out_specs=[vmem, vmem, vmem, vmem],
            scratch_shapes=[
                pltpu.VMEM((seqs, blk, head), BF16),
                pltpu.VMEM((seqs, blk, head), BF16),
                pltpu.VMEM((1, blk), jnp.int32),
                pltpu.VMEM((1, head), F32),
                pltpu.VMEM((mine, CORES, rows, head), BF16),
                pltpu.VMEM((mine, CORES, rows, head), BF16),
                pltpu.VMEM((mine, CORES * rows, head), BF16),
                pltpu.VMEM((CORES, 2, blk, head), F32),
                pltpu.VMEM((seqs, 2, blk, head), BF16),
                pltpu.VMEM((mine, cp, 2, blk, head), BF16),
                pltpu.VMEM((mine, keys, CORES * rows), BF16),
                pltpu.VMEM((mine, keys, CORES * rows), BF16),
                pltpu.VMEM((mine, cp, 2, blk, head), F32),
                pltpu.VMEM((mine, rows, head), BF16),
                pltpu.VMEM((mine, rows, head), BF16),
                dma((4,)), dma((2, mine)), dma((2, mine)), dma((2, mine)), dma, dma,
                dma((mine, chips, CORES)), dma((mine, cp)),
                dma((mine, 2, chips, CORES)), dma((chips, seqs, 2)),
                dma((2, mine)), dma((2, mine)),
            ],
            compiler_params=pltpu.CompilerParams(collective_id=0, has_side_effects=True,
                                                 vmem_limit_bytes=32 * 2 ** 20),
            name="attend",
        )(*(pltpu.with_memory_space_constraint(a, pltpu.HBM) for a in (
            query.reshape(seqs, rows, head), grad_out.reshape(seqs, rows, head), key, value,
            positions.reshape(1, blk), freq)))
        attn, dquery, dkey, dvalue = pl.pallas_call(
            finish_kernel,
            out_shape=[big, big, small, small],
            in_specs=[vmem] * 4,
            out_specs=[hbm, hbm, vmem, vmem],
            scratch_shapes=[dma((2,))],
            compiler_params=pltpu.CompilerParams(vmem_limit_bytes=16 * 2 ** 20),
            name="finish",
        )(o_mid, dq_mid, rbuf, tabs)
        shape = (seqs, blk, heads, head)
        return attn.reshape(shape), dquery.reshape(shape), dkey, dvalue

    return jax.shard_map(per_device, mesh=mesh, in_specs=(query_spec, kv_spec, kv_spec, pos_spec, query_spec),
                         out_specs=(query_spec, query_spec, kv_spec, kv_spec), check_vma=False)
```

```python
import functools

import jax
import jax.numpy as jnp
import numpy as np
from jax import lax
from jax.experimental import pallas as pl
from jax.experimental.pallas import tpu as pltpu
from jax.sharding import PartitionSpec as P

ROPE_BASE = 10000
CORES = 2
LOG2E = 1.4426950408889634
F32 = jnp.float32
BF16 = jnp.bfloat16
ROWS = 1024


def dot_nn(a, b):
    return jnp.dot(a, b, preferred_element_type=F32)


def dot_nt(a, b):
    return lax.dot_general(a, b, (((1,), (1,)), ((), ())), preferred_element_type=F32)


def attend_kernel(cp, blk, q_hbm, g_hbm, k_hbm, v_hbm, pos_hbm, freq_hbm,
                  o_ref, dq_ref, rbuf, tabs_out,
                  kv_in, pos_ref, freq_ref, qg, rq, tabs, kvown, kvb, g_t, tab_t, diff,
                  w_t, p_f, norm, p_t, ds_t, o_t, part, osib, dqsib,
                  first_sem, loc_sem, qg_send, qg_recv, tab_sem, kv_send, kv_recv,
                  r_sem, od_sem):
    chips = cp // CORES
    seqs = q_hbm.shape[0]
    mine = seqs // CORES
    rows, head = q_hbm.shape[1], q_hbm.shape[2]
    heads = rows // blk
    half_dim = head // 2
    keys = cp * blk
    scale = head ** -0.5
    me = lax.axis_index("cp")
    chip = lax.div(me, CORES)
    core = lax.rem(me, CORES)
    sib = chip * CORES + 1 - core

    barrier = pltpu.get_barrier_semaphore()
    for d in range(1, cp):
        pl.semaphore_signal(barrier, inc=1, device_id={"cp": lax.rem(me + d, cp)},
                            device_id_type=pl.DeviceIdType.MESH)

    def remote(src, dst, ssem, rsem, dev):
        return pltpu.make_async_remote_copy(src_ref=src, dst_ref=dst, send_sem=ssem, recv_sem=rsem,
                                            device_id={"cp": dev}, device_id_type=pl.DeviceIdType.MESH)

    def wait_bytes(ref, sem):
        pltpu.make_async_copy(ref, ref, sem).wait()

    def wait_by_chip(ref, sem, blocks):
        for c in range(chips):
            @pl.when(chip == c)
            def _():
                wait_bytes(ref.at[pl.ds(0, blocks(c))], sem)

    first = [pltpu.make_async_copy(pos_hbm, pos_ref, first_sem.at[0]),
             pltpu.make_async_copy(freq_hbm, freq_ref, first_sem.at[1]),
             pltpu.make_async_copy(k_hbm, kv_in.at[0], first_sem.at[2]),
             pltpu.make_async_copy(v_hbm, kv_in.at[1], first_sem.at[2])]
    for c in first:
        c.start()
    for n, src in enumerate((q_hbm, g_hbm)):
        for s in range(mine):
            pltpu.make_async_copy(src.at[core * mine + s], qg.at[n, s, 0], loc_sem).start()

    for d in range(1, chips):
        @pl.when(d > chip)
        def _():
            for n in range(2 * mine):
                kvb[n * cp + d * CORES:n * cp + (d + 1) * CORES] = jnp.zeros((CORES, blk, head), BF16)

        @pl.when(chip + d >= chips)
        def _():
            rbuf[d * seqs * 2:(d + 1) * seqs * 2] = jnp.zeros((seqs * 2, blk, head), F32)

    first[0].wait()
    first[1].wait()
    pos_row = jnp.broadcast_to(pos_ref[...].astype(F32), (blk, blk))
    ident = lax.broadcasted_iota(jnp.int32, (blk, blk), 0) == lax.broadcasted_iota(jnp.int32, (blk, blk), 1)
    pos_col = jnp.sum(jnp.where(ident, pos_row, 0.0), axis=1, keepdims=True)
    ang = pos_col * freq_ref[...]
    cos_t = jnp.cos(ang)
    lane = lax.broadcasted_iota(jnp.int32, (blk, head), 1)
    sin_t = jnp.where(lane < half_dim, -jnp.sin(ang), jnp.sin(ang))
    tabs[0, 0] = cos_t
    tabs[0, 1] = sin_t
    tabs_out[0] = cos_t
    tabs_out[1] = sin_t
    wait_bytes(kv_in, first_sem.at[2])
    for b in range(seqs):
        kf = kv_in[0, b].astype(F32)
        kvown[b, 0] = (kf * cos_t + pltpu.roll(kf, half_dim, 1) * sin_t).astype(BF16)
        kvown[b, 1] = kv_in[1, b]

    pl.semaphore_wait(barrier, cp - 1)

    def kv_wave(s, n):
        base = (s * 2 + n) * cp
        for d in range(chips - 1, 0, -1):
            @pl.when(chip + d < chips)
            def _():
                for k2 in range(CORES):
                    remote(kvown.at[k2 * mine + s, n], kvb.at[base + d * CORES + core], kv_send, kv_recv.at[s, n],
                           (chip + d) * CORES + k2).start()
        remote(kvown.at[(1 - core) * mine + s, n], kvb.at[base + core], kv_send, kv_recv.at[s, n], sib).start()

    def kv_wait(s, n):
        wait_by_chip(kvb, kv_recv.at[s, n], lambda c: CORES * c + 1)

    tab_copy = remote(tabs.at[0], tabs.at[1], tab_sem.at[0], tab_sem.at[1], sib)

    kv_wave(0, 0)
    tab_copy.start()
    for s in range(mine):
        for n, src in enumerate((q_hbm, g_hbm)):
            remote(src.at[(1 - core) * mine + s], qg.at[n, s, 1], qg_send, qg_recv.at[s], sib).start()
    for s in range(mine):
        for n in range(2):
            kvb[(s * 2 + n) * cp + core] = kvown[core * mine + s, n]

    def wide(tab):
        return jnp.broadcast_to(tab[:, None, :], (blk, heads, head)).reshape(rows, head)

    def prepare(s, h, cos_q, sin_q):
        x = qg[0, s, h].astype(F32)
        rq[s, h * rows:(h + 1) * rows, :] = (x * cos_q + pltpu.roll(x, half_dim, 1) * sin_q).astype(BF16)
        g_t[s, :, h * rows:(h + 1) * rows] = qg[1, s, h].T

    def tables(h):
        cos_b, sin_b = tabs[h, 0], tabs[h, 1]
        tab_t[:, h * rows:(h + 1) * rows] = wide(jnp.where(lane < half_dim, cos_b, sin_b) * scale).T
        return wide(cos_b), wide(sin_b)

    diff[...] = lax.broadcasted_iota(jnp.int32, (blk, rows), 0) - lax.div(
        lax.broadcasted_iota(jnp.int32, (blk, rows), 1), heads)
    wait_bytes(qg.at[0], loc_sem)
    cs = tables(0)
    prepare(0, 0, *cs)
    kv_wave(0, 1)
    for s in range(1, mine):
        prepare(s, 0, *cs)
    tab_copy.wait_recv()
    cs = tables(1)
    for s in range(mine):
        wait_bytes(qg.at[0, 0], qg_recv.at[s])
        prepare(s, 1, *cs)
        if s + 1 < mine:
            kv_wave(s + 1, 0)
    for s in range(1, mine):
        kv_wave(s, 1)

    def send_part(s, x):
        base = (s * 2 + x) * cp
        slot = (core * mine + s) * 2 + x
        for d in range(chips - 1, 0, -1):
            @pl.when(chip >= d)
            def _():
                for k2 in range(CORES):
                    remote(part.at[base + d * CORES + k2], rbuf.at[d * seqs * 2 + slot], r_sem.at[0], r_sem.at[1],
                           (chip - d) * CORES + k2).start()
        remote(part.at[base + 1 - core], rbuf.at[slot], r_sem.at[0], r_sem.at[1], sib).start()
        rbuf[slot] = part[base + core]

    def out_copy(src, dst, s):
        return remote(src.at[s], dst.at[core * mine + s], od_sem.at[0], od_sem.at[1], sib)

    for s in range(mine):
        kv_wait(s, 0)
        kk = kvb[s * 2 * cp:(s * 2 + 1) * cp].reshape(keys, head)
        for h in (1, 0):
            owner = core if h == 0 else 1 - core
            for r in range(0, rows, ROWS):
                row0 = h * rows + r
                x = dot_nt(kk, rq[s, row0:row0 + ROWS, :])
                dif = diff[:, r:r + ROWS]
                pieces = [jnp.where(dif <= (owner - k) * blk, x[k * blk:(k + 1) * blk], -jnp.inf)
                          for k in range(CORES)]
                for d in range(1, chips):
                    bias = jnp.where(d <= chip, 0.0, -jnp.inf)
                    pieces.append(x[d * CORES * blk:(d + 1) * CORES * blk] + bias)
                x = jnp.concatenate(pieces, axis=0)
                mx = jnp.max(x, axis=0, keepdims=True)
                w = jnp.exp2((x - mx) * (scale * LOG2E))
                inv_l = 1.0 / jnp.sum(w, axis=0, keepdims=True)
                w_t[:, row0:row0 + ROWS] = w.astype(BF16)
                p = w * inv_l
                p_f[:, row0:row0 + ROWS] = p
                p_t[:, row0:row0 + ROWS] = p.astype(BF16)
                norm[:, row0:row0 + ROWS] = inv_l
        part[(s * 2 + 1) * cp:(s * 2 + 2) * cp] = dot_nn(
            p_t[...], qg[1, s].reshape(CORES * rows, head)).reshape(cp, blk, head)
        send_part(s, 1)
        kv_wait(s, 1)
        vv = kvb[(s * 2 + 1) * cp:(s * 2 + 2) * cp].reshape(keys, head)
        v_t = vv.T
        for h in (1, 0):
            for r in range(0, rows, ROWS):
                row0 = h * rows + r
                ot = (dot_nn(v_t, w_t[:, row0:row0 + ROWS]) * norm[:, row0:row0 + ROWS]).astype(BF16)
                o_t[s, :, row0:row0 + ROWS] = ot
                delta = jnp.sum(g_t[s, :, row0:row0 + ROWS].astype(F32) * ot.astype(F32), axis=0, keepdims=True)
                dp = dot_nt(vv, qg[1, s, h, r:r + ROWS, :])
                ds_t[s, :, row0:row0 + ROWS] = (p_f[:, row0:row0 + ROWS] * (dp - delta)).astype(BF16)
        part[s * 2 * cp:(s * 2 + 1) * cp] = dot_nn(ds_t[s], rq[s]).reshape(cp, blk, head)
        send_part(s, 0)

    for s in range(mine):
        k_t = kvb[s * 2 * cp:(s * 2 + 1) * cp].reshape(keys, head).T
        for h in (1, 0):
            for r in range(0, rows, ROWS):
                row0 = h * rows + r
                dq_t = dot_nn(k_t, ds_t[s, :, row0:row0 + ROWS])
                cos_q = tab_t[:half_dim, row0:row0 + ROWS]
                sin_q = tab_t[half_dim:, row0:row0 + ROWS]
                top, low = dq_t[:half_dim], dq_t[half_dim:]
                dq = jnp.concatenate([top * cos_q + low * sin_q, low * cos_q - top * sin_q], axis=0).astype(BF16).T
                out = o_t[s, :, row0:row0 + ROWS].T
                if h == 0:
                    dq_ref[core * mine + s, r:r + ROWS, :] = dq
                    o_ref[core * mine + s, r:r + ROWS, :] = out
                else:
                    dqsib[s, r:r + ROWS, :] = dq
                    osib[s, r:r + ROWS, :] = out
            if h == 1:
                out_copy(osib, o_ref, s).start()
                out_copy(dqsib, dq_ref, s).start()

    tab_copy.wait_send()
    wait_bytes(qg.at[0], qg_send)
    wait_by_chip(kvb, kv_send, lambda c: 2 * mine * (CORES * (chips - 1 - c) + 1))
    wait_bytes(qg.at[0], od_sem.at[0])
    wait_bytes(qg.at[0], od_sem.at[1])
    wait_by_chip(part, r_sem.at[0], lambda c: 2 * mine * (CORES * c + 1))
    wait_by_chip(rbuf, r_sem.at[1], lambda c: 2 * mine * (CORES * (chips - 1 - c) + 1))


def finish_kernel(o_in, dq_in, rbuf, tabs, o_hbm, dq_hbm, dk_hbm, dv_hbm, dk_buf, dv_buf, sem):
    copies = [pltpu.make_async_copy(o_in, o_hbm, sem.at[0]), pltpu.make_async_copy(dq_in, dq_hbm, sem.at[1]),
              pltpu.make_async_copy(dk_buf, dk_hbm, sem.at[2]), pltpu.make_async_copy(dv_buf, dv_hbm, sem.at[3])]
    for c in copies[:2]:
        c.start()
    head = tabs.shape[-1]
    scale = head ** -0.5
    cos_t, sin_t = tabs[0], tabs[1]
    seqs = dk_buf.shape[0]
    for b in range(seqs):
        dk = rbuf[2 * b]
        dv = rbuf[2 * b + 1]
        for c in range(2 * seqs, rbuf.shape[0], 2 * seqs):
            dk = dk + rbuf[c + 2 * b]
            dv = dv + rbuf[c + 2 * b + 1]
        dk = dk * scale
        dk_buf[b] = (dk * cos_t - pltpu.roll(dk, head // 2, 1) * sin_t).astype(BF16)
        dv_buf[b] = dv.astype(BF16)
    for c in copies[2:]:
        c.start()
    for c in copies:
        c.wait()


def solution(mesh):
    cp = mesh.shape["cp"]
    query_spec = P("dp", "cp", None, None)
    kv_spec = P("dp", "cp", None)
    pos_spec = P(("dp", "cp"))

    def per_device(query, key, value, positions, grad_out):
        seqs, blk, heads, head = query.shape
        rows = blk * heads
        chips = cp // CORES
        mine = seqs // CORES
        keys = cp * blk
        freq = np.power(float(ROPE_BASE), -2.0 * np.arange(head // 2) / head)
        freq = jnp.asarray(np.concatenate([freq, freq])[None, :].astype(np.float32))
        vmem = pl.BlockSpec(memory_space=pltpu.VMEM)
        hbm = pl.BlockSpec(memory_space=pltpu.HBM)
        dma = pltpu.SemaphoreType.DMA
        big = jax.ShapeDtypeStruct((seqs, rows, head), BF16)
        small = jax.ShapeDtypeStruct((seqs, blk, head), BF16)
        o_mid, dq_mid, rbuf, tabs = pl.pallas_call(
            functools.partial(attend_kernel, cp, blk),
            out_shape=[big, big, jax.ShapeDtypeStruct((chips * seqs * 2, blk, head), F32),
                       jax.ShapeDtypeStruct((2, blk, head), F32)],
            in_specs=[hbm] * 6,
            out_specs=[vmem, vmem, vmem, vmem],
            scratch_shapes=[
                pltpu.VMEM((2, seqs, blk, head), BF16),
                pltpu.VMEM((1, blk), jnp.int32),
                pltpu.VMEM((1, head), F32),
                pltpu.VMEM((2, mine, CORES, rows, head), BF16),
                pltpu.VMEM((mine, CORES * rows, head), BF16),
                pltpu.VMEM((CORES, 2, blk, head), F32),
                pltpu.VMEM((seqs, 2, blk, head), BF16),
                pltpu.VMEM((mine * 2 * cp, blk, head), BF16),
                pltpu.VMEM((mine, head, CORES * rows), BF16),
                pltpu.VMEM((head, CORES * rows), F32),
                pltpu.VMEM((blk, rows), jnp.int32),
                pltpu.VMEM((keys, CORES * rows), BF16),
                pltpu.VMEM((keys, CORES * rows), F32),
                pltpu.VMEM((1, CORES * rows), F32),
                pltpu.VMEM((keys, CORES * rows), BF16),
                pltpu.VMEM((mine, keys, CORES * rows), BF16),
                pltpu.VMEM((mine, head, CORES * rows), BF16),
                pltpu.VMEM((mine * 2 * cp, blk, head), F32),
                pltpu.VMEM((mine, rows, head), BF16),
                pltpu.VMEM((mine, rows, head), BF16),
                dma((3,)), dma, dma, dma((mine,)), dma((2,)), dma, dma((mine, 2)), dma((2,)), dma((2,)),
            ],
            compiler_params=pltpu.CompilerParams(collective_id=0, has_side_effects=True,
                                                 vmem_limit_bytes=32 * 2 ** 20),
            name="attend",
        )(*(pltpu.with_memory_space_constraint(a, pltpu.HBM) for a in (
            query.reshape(seqs, rows, head), grad_out.reshape(seqs, rows, head), key, value,
            positions.reshape(1, blk), freq)))
        attn, dquery, dkey, dvalue = pl.pallas_call(
            finish_kernel,
            out_shape=[big, big, small, small],
            in_specs=[vmem] * 4,
            out_specs=[hbm] * 4,
            scratch_shapes=[pltpu.VMEM((seqs, blk, head), BF16), pltpu.VMEM((seqs, blk, head), BF16), dma((4,))],
            compiler_params=pltpu.CompilerParams(vmem_limit_bytes=16 * 2 ** 20),
            name="finish",
        )(o_mid, dq_mid, rbuf, tabs)
        shape = (seqs, blk, heads, head)
        return attn.reshape(shape), dquery.reshape(shape), dkey, dvalue

    return jax.shard_map(per_device, mesh=mesh, in_specs=(query_spec, kv_spec, kv_spec, pos_spec, query_spec),
                         out_specs=(query_spec, query_spec, kv_spec, kv_spec), check_vma=False)
```

```python
import functools

import jax
import jax.numpy as jnp
import numpy as np
from jax import lax
from jax.experimental import pallas as pl
from jax.experimental.pallas import tpu as pltpu
from jax.sharding import PartitionSpec as P

ROPE_BASE = 10000
CORES = 2
LOG2E = 1.4426950408889634
F32 = jnp.float32
BF16 = jnp.bfloat16
ROWS = 512
LANES = 128
RELAYED = (1,)


def dot_nn(a, b):
    return jnp.dot(a, b, preferred_element_type=F32)


def dot_nt(a, b):
    return lax.dot_general(a, b, (((1,), (1,)), ((), ())), preferred_element_type=F32)


def put(ref, row0, val):
    for n in range(0, val.shape[1], LANES):
        ref[(row0 + n) // LANES] = val[:, n:n + LANES]


def get(ref, row0, count):
    return jnp.concatenate([ref[(row0 + n) // LANES] for n in range(0, count, LANES)], axis=1)


def attend_kernel(cp, blk, q_hbm, g_hbm, k_hbm, v_hbm, pos_hbm, freq_hbm,
                  o_ref, dq_ref, rbuf, tabs_out,
                  kv_in, pos_ref, freq_ref, qg, rq, tabs, kvown, kvb, g_t, tab_t, diff,
                  w_t, p_f, norm, p_t, ds_t, o_t, part, passing, osib, dqsib,
                  first_sem, loc_sem, qg_send, qg_recv, tab_sem, kv_send, kv_recv,
                  r_sem, pass_sem, od_sem):
    chips = cp // CORES
    seqs = q_hbm.shape[0]
    mine = seqs // CORES
    rows, head = q_hbm.shape[1], q_hbm.shape[2]
    heads = rows // blk
    half_dim = head // 2
    keys = cp * blk
    scale = head ** -0.5
    me = lax.axis_index("cp")
    chip = lax.div(me, CORES)
    core = lax.rem(me, CORES)
    sib = chip * CORES + 1 - core

    barrier = pltpu.get_barrier_semaphore()
    for d in range(1, cp):
        pl.semaphore_signal(barrier, inc=1, device_id={"cp": lax.rem(me + d, cp)},
                            device_id_type=pl.DeviceIdType.MESH)

    def remote(src, dst, ssem, rsem, dev):
        return pltpu.make_async_remote_copy(src_ref=src, dst_ref=dst, send_sem=ssem, recv_sem=rsem,
                                            device_id={"cp": dev}, device_id_type=pl.DeviceIdType.MESH)

    def wait_bytes(ref, sem):
        pltpu.make_async_copy(ref, ref, sem).wait()

    def wait_by_chip(ref, sem, blocks):
        for c in range(chips):
            @pl.when(chip == c)
            def _():
                wait_bytes(ref.at[pl.ds(0, blocks(c))], sem)

    first = [pltpu.make_async_copy(pos_hbm, pos_ref, first_sem.at[0]),
             pltpu.make_async_copy(freq_hbm, freq_ref, first_sem.at[1]),
             pltpu.make_async_copy(k_hbm, kv_in.at[0], first_sem.at[2]),
             pltpu.make_async_copy(v_hbm, kv_in.at[1], first_sem.at[2])]
    for c in first:
        c.start()
    for n, src in enumerate((q_hbm, g_hbm)):
        for s in range(mine):
            pltpu.make_async_copy(src.at[core * mine + s], qg.at[n, s, 0], loc_sem).start()

    for d in range(1, chips):
        @pl.when(d > chip)
        def _():
            for n in range(2 * mine):
                kvb[n * cp + d * CORES:n * cp + (d + 1) * CORES] = jnp.zeros((CORES, blk, head), BF16)

        if d == chips - 2:
            @pl.when(chip == 0)
            def _():
                for k2 in range(CORES):
                    for x in RELAYED:
                        rbuf[(d * seqs + k2 * mine) * 2 + x] = jnp.zeros((blk, head), F32)

        @pl.when(chip + d >= chips)
        def _():
            rbuf[d * seqs * 2:(d + 1) * seqs * 2] = jnp.zeros((seqs * 2, blk, head), F32)

    first[0].wait()
    first[1].wait()
    pos_row = jnp.broadcast_to(pos_ref[...].astype(F32), (blk, blk))
    ident = lax.broadcasted_iota(jnp.int32, (blk, blk), 0) == lax.broadcasted_iota(jnp.int32, (blk, blk), 1)
    pos_col = jnp.sum(jnp.where(ident, pos_row, 0.0), axis=1, keepdims=True)
    ang = pos_col * freq_ref[...]
    cos_t = jnp.cos(ang)
    lane = lax.broadcasted_iota(jnp.int32, (blk, head), 1)
    sin_t = jnp.where(lane < half_dim, -jnp.sin(ang), jnp.sin(ang))
    tabs[0, 0] = cos_t
    tabs[0, 1] = sin_t
    tabs_out[0] = cos_t
    tabs_out[1] = sin_t
    wait_bytes(kv_in, first_sem.at[2])
    for b in range(seqs):
        kf = kv_in[0, b].astype(F32)
        kvown[b, 0] = (kf * cos_t + pltpu.roll(kf, half_dim, 1) * sin_t).astype(BF16)
        kvown[b, 1] = kv_in[1, b]

    pl.semaphore_wait(barrier, cp - 1)

    def kv_wave(s, n):
        base = (s * 2 + n) * cp
        for d in range(chips - 1, 0, -1):
            @pl.when(chip + d < chips)
            def _():
                for k2 in range(CORES):
                    remote(kvown.at[k2 * mine + s, n], kvb.at[base + d * CORES + core], kv_send, kv_recv.at[s, n],
                           (chip + d) * CORES + k2).start()
        remote(kvown.at[(1 - core) * mine + s, n], kvb.at[base + core], kv_send, kv_recv.at[s, n], sib).start()

    def kv_wait(s, n):
        wait_by_chip(kvb, kv_recv.at[s, n], lambda c: CORES * c + 1)

    tab_copy = remote(tabs.at[0], tabs.at[1], tab_sem.at[0], tab_sem.at[1], sib)

    kv_wave(0, 0)
    tab_copy.start()
    for s in range(mine):
        for n, src in enumerate((q_hbm, g_hbm)):
            remote(src.at[(1 - core) * mine + s], qg.at[n, s, 1], qg_send, qg_recv.at[s], sib).start()
    for s in range(mine):
        for n in range(2):
            kvb[(s * 2 + n) * cp + core] = kvown[core * mine + s, n]

    def wide(tab):
        return jnp.broadcast_to(tab[:, None, :], (blk, heads, head)).reshape(rows, head)

    def prepare(s, h, cos_q, sin_q):
        x = qg[0, s, h].astype(F32)
        rq[s, h * rows:(h + 1) * rows, :] = (x * cos_q + pltpu.roll(x, half_dim, 1) * sin_q).astype(BF16)
        put(g_t.at[s], h * rows, qg[1, s, h].T)

    def tables(h):
        cos_b, sin_b = tabs[h, 0], tabs[h, 1]
        put(tab_t, h * rows, wide(jnp.where(lane < half_dim, cos_b, sin_b) * scale).T)
        return wide(cos_b), wide(sin_b)

    put(diff, 0, lax.broadcasted_iota(jnp.int32, (blk, rows), 0) - lax.div(
        lax.broadcasted_iota(jnp.int32, (blk, rows), 1), heads))
    wait_bytes(qg.at[0], loc_sem)
    cs = tables(0)
    prepare(0, 0, *cs)
    kv_wave(0, 1)
    for s in range(1, mine):
        prepare(s, 0, *cs)
    tab_copy.wait_recv()
    cs = tables(1)
    for s in range(mine):
        wait_bytes(qg.at[0, 0], qg_recv.at[s])
        prepare(s, 1, *cs)
        if s + 1 < mine:
            kv_wave(s + 1, 0)
    for s in range(1, mine):
        kv_wave(s, 1)

    origin = chips - 2
    middle = origin - 1

    def send_far(s, x, d):
        base = (s * 2 + x) * cp
        slot = (core * mine + s) * 2 + x
        for k2 in range(CORES):
            remote(part.at[base + d * CORES + k2], rbuf.at[d * seqs * 2 + slot], r_sem.at[0], r_sem.at[1],
                   (chip - d) * CORES + k2).start()

    def send_part(s, x):
        base = (s * 2 + x) * cp
        slot = (core * mine + s) * 2 + x
        relayed = s == 0 and x in RELAYED
        for d in range(chips - 1, 0, -1):
            direct = chip >= d
            if relayed and d == origin:
                direct = jnp.logical_and(direct, chip != origin)

                @pl.when(chip == origin)
                def _():
                    n = RELAYED.index(x) * CORES
                    for k2 in range(CORES):
                        remote(part.at[base + d * CORES + k2], passing.at[n + k2], r_sem.at[0], pass_sem,
                               middle * CORES + core).start()
            if relayed and d == middle:
                direct = jnp.logical_and(direct, chip != middle)

            @pl.when(direct)
            def _():
                send_far(s, x, d)
        remote(part.at[base + 1 - core], rbuf.at[slot], r_sem.at[0], r_sem.at[1], sib).start()
        rbuf[slot] = part[base + core]

    def out_copy(src, dst, s):
        return remote(src.at[s], dst.at[core * mine + s], od_sem.at[0], od_sem.at[1], sib)

    for s in range(mine):
        kv_wait(s, 0)
        kk = kvb[s * 2 * cp:(s * 2 + 1) * cp].reshape(keys, head)
        for h in (0, 1):
            owner = core if h == 0 else 1 - core
            for r in range(0, rows, ROWS):
                row0 = h * rows + r
                x = dot_nt(kk, rq[s, row0:row0 + ROWS, :])
                dif = get(diff, r, ROWS)
                pieces = [jnp.where(dif <= (owner - k) * blk, x[k * blk:(k + 1) * blk], -jnp.inf)
                          for k in range(CORES)]
                for d in range(1, chips):
                    bias = jnp.where(d <= chip, 0.0, -jnp.inf)
                    pieces.append(x[d * CORES * blk:(d + 1) * CORES * blk] + bias)
                x = jnp.concatenate(pieces, axis=0)
                mx = jnp.max(x, axis=0, keepdims=True)
                w = jnp.exp2((x - mx) * (scale * LOG2E))
                inv_l = 1.0 / jnp.sum(w, axis=0, keepdims=True)
                put(w_t, row0, w.astype(BF16))
                p = w * inv_l
                put(p_f, row0, p)
                put(p_t, row0, p.astype(BF16))
                norm[:, row0:row0 + ROWS] = inv_l
        part[(s * 2 + 1) * cp:(s * 2 + 2) * cp] = dot_nn(
            get(p_t, 0, CORES * rows), qg[1, s].reshape(CORES * rows, head)).reshape(cp, blk, head)
        send_part(s, 1)
        kv_wait(s, 1)
        vv = kvb[(s * 2 + 1) * cp:(s * 2 + 2) * cp].reshape(keys, head)
        v_t = vv.T
        for h in (0, 1):
            for r in range(0, rows, ROWS):
                row0 = h * rows + r
                ot = (dot_nn(v_t, get(w_t, row0, ROWS)) * norm[:, row0:row0 + ROWS]).astype(BF16)
                put(o_t.at[s], row0, ot)
                delta = jnp.sum(get(g_t.at[s], row0, ROWS).astype(F32) * ot.astype(F32), axis=0, keepdims=True)
                dp = dot_nt(vv, qg[1, s, h, r:r + ROWS, :])
                put(ds_t.at[s], row0, (get(p_f, row0, ROWS) * (dp - delta)).astype(BF16))
        part[s * 2 * cp:(s * 2 + 1) * cp] = dot_nn(get(ds_t.at[s], 0, CORES * rows), rq[s]).reshape(cp, blk, head)
        send_part(s, 0)

    @pl.when(chip == middle)
    def _():
        wait_bytes(passing, pass_sem)
        for n, x in enumerate(RELAYED):
            first_slot = x * cp + middle * CORES
            part[first_slot:first_slot + CORES] += passing[n * CORES:(n + 1) * CORES]
            send_far(0, x, middle)

    for s in range(mine):
        k_t = kvb[s * 2 * cp:(s * 2 + 1) * cp].reshape(keys, head).T
        for h in (1, 0):
            for r in range(0, rows, ROWS):
                row0 = h * rows + r
                dq_t = dot_nn(k_t, get(ds_t.at[s], row0, ROWS))
                tab = get(tab_t, row0, ROWS)
                cos_q, sin_q = tab[:half_dim], tab[half_dim:]
                top, low = dq_t[:half_dim], dq_t[half_dim:]
                dq = jnp.concatenate([top * cos_q + low * sin_q, low * cos_q - top * sin_q], axis=0).astype(BF16).T
                out = get(o_t.at[s], row0, ROWS).T
                if h == 0:
                    dq_ref[core * mine + s, r:r + ROWS, :] = dq
                    o_ref[core * mine + s, r:r + ROWS, :] = out
                else:
                    dqsib[s, r:r + ROWS, :] = dq
                    osib[s, r:r + ROWS, :] = out
            if h == 1:
                out_copy(osib, o_ref, s).start()
                out_copy(dqsib, dq_ref, s).start()

    tab_copy.wait_send()
    wait_bytes(qg.at[0], qg_send)
    wait_by_chip(kvb, kv_send, lambda c: 2 * mine * (CORES * (chips - 1 - c) + 1))
    wait_bytes(qg.at[0], od_sem.at[0])
    wait_bytes(qg.at[0], od_sem.at[1])
    wait_by_chip(part, r_sem.at[0], lambda c: 2 * mine * (CORES * c + 1))
    wait_by_chip(rbuf, r_sem.at[1], lambda c: 2 * mine * (CORES * (chips - 1 - c) + 1)
                 - (CORES * len(RELAYED) if c == 0 else 0))


def finish_kernel(o_in, dq_in, rbuf, tabs, o_hbm, dq_hbm, dk_hbm, dv_hbm, dk_buf, dv_buf, sem):
    copies = [pltpu.make_async_copy(o_in, o_hbm, sem.at[0]), pltpu.make_async_copy(dq_in, dq_hbm, sem.at[1]),
              pltpu.make_async_copy(dk_buf, dk_hbm, sem.at[2]), pltpu.make_async_copy(dv_buf, dv_hbm, sem.at[3])]
    for c in copies[:2]:
        c.start()
    head = tabs.shape[-1]
    scale = head ** -0.5
    cos_t, sin_t = tabs[0], tabs[1]
    seqs = dk_buf.shape[0]
    for b in range(seqs):
        dk = rbuf[2 * b]
        dv = rbuf[2 * b + 1]
        for c in range(2 * seqs, rbuf.shape[0], 2 * seqs):
            dk = dk + rbuf[c + 2 * b]
            dv = dv + rbuf[c + 2 * b + 1]
        dk = dk * scale
        dk_buf[b] = (dk * cos_t - pltpu.roll(dk, head // 2, 1) * sin_t).astype(BF16)
        dv_buf[b] = dv.astype(BF16)
    for c in copies[2:]:
        c.start()
    for c in copies:
        c.wait()


def solution(mesh):
    cp = mesh.shape["cp"]
    query_spec = P("dp", "cp", None, None)
    kv_spec = P("dp", "cp", None)
    pos_spec = P(("dp", "cp"))

    def per_device(query, key, value, positions, grad_out):
        seqs, blk, heads, head = query.shape
        rows = blk * heads
        chips = cp // CORES
        mine = seqs // CORES
        keys = cp * blk
        tiles = CORES * rows // LANES
        freq = np.power(float(ROPE_BASE), -2.0 * np.arange(head // 2) / head)
        freq = jnp.asarray(np.concatenate([freq, freq])[None, :].astype(np.float32))
        vmem = pl.BlockSpec(memory_space=pltpu.VMEM)
        hbm = pl.BlockSpec(memory_space=pltpu.HBM)
        dma = pltpu.SemaphoreType.DMA
        big = jax.ShapeDtypeStruct((seqs, rows, head), BF16)
        small = jax.ShapeDtypeStruct((seqs, blk, head), BF16)
        o_mid, dq_mid, rbuf, tabs = pl.pallas_call(
            functools.partial(attend_kernel, cp, blk),
            out_shape=[big, big, jax.ShapeDtypeStruct((chips * seqs * 2, blk, head), F32),
                       jax.ShapeDtypeStruct((2, blk, head), F32)],
            in_specs=[hbm] * 6,
            out_specs=[vmem, vmem, vmem, vmem],
            scratch_shapes=[
                pltpu.VMEM((2, seqs, blk, head), BF16),
                pltpu.VMEM((1, blk), jnp.int32),
                pltpu.VMEM((1, head), F32),
                pltpu.VMEM((2, mine, CORES, rows, head), BF16),
                pltpu.VMEM((mine, CORES * rows, head), BF16),
                pltpu.VMEM((CORES, 2, blk, head), F32),
                pltpu.VMEM((seqs, 2, blk, head), BF16),
                pltpu.VMEM((mine * 2 * cp, blk, head), BF16),
                pltpu.VMEM((mine, tiles, head, LANES), BF16),
                pltpu.VMEM((tiles, head, LANES), F32),
                pltpu.VMEM((tiles, blk, LANES), jnp.int32),
                pltpu.VMEM((tiles, keys, LANES), BF16),
                pltpu.VMEM((tiles, keys, LANES), F32),
                pltpu.VMEM((1, CORES * rows), F32),
                pltpu.VMEM((tiles, keys, LANES), BF16),
                pltpu.VMEM((mine, tiles, keys, LANES), BF16),
                pltpu.VMEM((mine, tiles, head, LANES), BF16),
                pltpu.VMEM((mine * 2 * cp, blk, head), F32),
                pltpu.VMEM((CORES * len(RELAYED), blk, head), F32),
                pltpu.VMEM((mine, rows, head), BF16),
                pltpu.VMEM((mine, rows, head), BF16),
                dma((3,)), dma, dma, dma((mine,)), dma((2,)), dma, dma((mine, 2)), dma((2,)), dma, dma((2,)),
            ],
            compiler_params=pltpu.CompilerParams(collective_id=0, has_side_effects=True,
                                                 vmem_limit_bytes=32 * 2 ** 20),
            name="attend",
        )(*(pltpu.with_memory_space_constraint(a, pltpu.HBM) for a in (
            query.reshape(seqs, rows, head), grad_out.reshape(seqs, rows, head), key, value,
            positions.reshape(1, blk), freq)))
        attn, dquery, dkey, dvalue = pl.pallas_call(
            finish_kernel,
            out_shape=[big, big, small, small],
            in_specs=[vmem] * 4,
            out_specs=[hbm] * 4,
            scratch_shapes=[pltpu.VMEM((seqs, blk, head), BF16), pltpu.VMEM((seqs, blk, head), BF16), dma((4,))],
            compiler_params=pltpu.CompilerParams(vmem_limit_bytes=16 * 2 ** 20),
            name="finish",
        )(o_mid, dq_mid, rbuf, tabs)
        shape = (seqs, blk, heads, head)
        return attn.reshape(shape), dquery.reshape(shape), dkey, dvalue

    return jax.shard_map(per_device, mesh=mesh, in_specs=(query_spec, kv_spec, kv_spec, pos_spec, query_spec),
                         out_specs=(query_spec, query_spec, kv_spec, kv_spec), check_vma=False)
```

```python
import functools

import jax
import jax.numpy as jnp
import numpy as np
from jax import lax
from jax.experimental import pallas as pl
from jax.experimental.pallas import tpu as pltpu
from jax.sharding import PartitionSpec as P

ROPE_BASE = 10000
CORES = 2
LOG2E = 1.4426950408889634
F32 = jnp.float32
BF16 = jnp.bfloat16
ROWS = 512
LANES = 128
RELAYED = (0,)


def dot_nn(a, b):
    return jnp.dot(a, b, preferred_element_type=F32)


def dot_nt(a, b):
    return lax.dot_general(a, b, (((1,), (1,)), ((), ())), preferred_element_type=F32)


def put(ref, row0, val):
    for n in range(0, val.shape[1], LANES):
        ref[(row0 + n) // LANES, :val.shape[0]] = val[:, n:n + LANES]


def get(ref, row0, count, height=None):
    height = ref.shape[1] if height is None else height
    return jnp.concatenate([ref[(row0 + n) // LANES, :height] for n in range(0, count, LANES)], axis=1)


def attend_kernel(cp, blk, q_hbm, g_hbm, k_hbm, v_hbm, pos_hbm, freq_hbm,
                  o_ref, dq_ref, rbuf, tabs_out,
                  kv_in, pos_ref, freq_ref, qg, rq, tabs, kvown, kvb, g_t, tab_t, diff,
                  x_s, w_t, p_f, norm, p_t, ds_t, o_t, part, passing, osib, dqsib,
                  first_sem, loc_sem, qg_send, qg_recv, tab_sem, kv_send, kv_recv, far_recv,
                  r_sem, pass_sem, od_sem):
    chips = cp // CORES
    seqs = q_hbm.shape[0]
    mine = seqs // CORES
    rows, head = q_hbm.shape[1], q_hbm.shape[2]
    heads = rows // blk
    half_dim = head // 2
    keys = cp * blk
    scale = head ** -0.5
    me = lax.axis_index("cp")
    chip = lax.div(me, CORES)
    core = lax.rem(me, CORES)
    sib = chip * CORES + 1 - core

    barrier = pltpu.get_barrier_semaphore()
    for d in range(1, cp):
        pl.semaphore_signal(barrier, inc=1, device_id={"cp": lax.rem(me + d, cp)},
                            device_id_type=pl.DeviceIdType.MESH)

    def remote(src, dst, ssem, rsem, dev):
        return pltpu.make_async_remote_copy(src_ref=src, dst_ref=dst, send_sem=ssem, recv_sem=rsem,
                                            device_id={"cp": dev}, device_id_type=pl.DeviceIdType.MESH)

    def wait_bytes(ref, sem):
        pltpu.make_async_copy(ref, ref, sem).wait()

    def wait_by_chip(ref, sem, blocks, last=None):
        if last:
            wait_bytes(ref.at[pl.ds(0, blocks(chips - 1))], sem)
            return
        for c in range(chips if last is None else chips - 1):
            if blocks(c):
                @pl.when(chip == c)
                def _():
                    wait_bytes(ref.at[pl.ds(0, blocks(c))], sem)

    first = [pltpu.make_async_copy(pos_hbm, pos_ref, first_sem.at[0]),
             pltpu.make_async_copy(freq_hbm, freq_ref, first_sem.at[1]),
             pltpu.make_async_copy(k_hbm, kv_in.at[0], first_sem.at[2]),
             pltpu.make_async_copy(v_hbm, kv_in.at[1], first_sem.at[2])]
    for c in first:
        c.start()
    for n, src in enumerate((q_hbm, g_hbm)):
        for s in range(mine):
            pltpu.make_async_copy(src.at[core * mine + s], qg.at[n, s, 0], loc_sem).start()

    for d in range(1, chips):
        @pl.when(d > chip)
        def _():
            for n in range(2 * mine):
                kvb[n * cp + d * CORES:n * cp + (d + 1) * CORES] = jnp.zeros((CORES, blk, head), BF16)

        if d == chips - 2:
            @pl.when(chip == 0)
            def _():
                for k2 in range(CORES):
                    for x in RELAYED:
                        rbuf[(d * seqs + k2 * mine) * 2 + x] = jnp.zeros((blk, head), F32)

        @pl.when(chip + d >= chips)
        def _():
            rbuf[d * seqs * 2:(d + 1) * seqs * 2] = jnp.zeros((seqs * 2, blk, head), F32)

    @pl.when(chip < chips - 1)
    def _():
        ds_t[:, :, keys - CORES * blk:] = jnp.zeros((mine, ds_t.shape[1], CORES * blk, LANES), BF16)

    first[0].wait()
    first[1].wait()
    pos_row = jnp.broadcast_to(pos_ref[...].astype(F32), (blk, blk))
    ident = lax.broadcasted_iota(jnp.int32, (blk, blk), 0) == lax.broadcasted_iota(jnp.int32, (blk, blk), 1)
    pos_col = jnp.sum(jnp.where(ident, pos_row, 0.0), axis=1, keepdims=True)
    ang = pos_col * freq_ref[...]
    cos_t = jnp.cos(ang)
    lane = lax.broadcasted_iota(jnp.int32, (blk, head), 1)
    sin_t = jnp.where(lane < half_dim, -jnp.sin(ang), jnp.sin(ang))
    tabs[0, 0] = cos_t
    tabs[0, 1] = sin_t
    tabs_out[0] = cos_t
    tabs_out[1] = sin_t
    wait_bytes(kv_in, first_sem.at[2])
    for b in range(seqs):
        kf = kv_in[0, b].astype(F32)
        kvown[b, 0] = (kf * cos_t + pltpu.roll(kf, half_dim, 1) * sin_t).astype(BF16)
        kvown[b, 1] = kv_in[1, b]

    pl.semaphore_wait(barrier, cp - 1)

    def kv_wave(s, n):
        base = (s * 2 + n) * cp
        for d in range(chips - 1, 0, -1):
            @pl.when(chip + d < chips)
            def _():
                for k2 in range(CORES):
                    remote(kvown.at[k2 * mine + s, n], kvb.at[base + d * CORES + core], kv_send,
                           far_recv if (s, n) == (0, 0) and d > 1 else kv_recv.at[s, n],
                           (chip + d) * CORES + k2).start()
        remote(kvown.at[(1 - core) * mine + s, n], kvb.at[base + core], kv_send, kv_recv.at[s, n], sib).start()

    def kv_wait(s, n, last):
        wait_by_chip(kvb, kv_recv.at[s, n], lambda c: CORES * (min(c, 1) if (s, n) == (0, 0) else c) + 1, last)

    def far_wait(last):
        wait_by_chip(kvb, far_recv, lambda c: CORES * max(c - 1, 0), last)

    tab_copy = remote(tabs.at[0], tabs.at[1], tab_sem.at[0], tab_sem.at[1], sib)

    kv_wave(0, 0)
    tab_copy.start()
    for s in range(mine):
        for n, src in enumerate((q_hbm, g_hbm)):
            remote(src.at[(1 - core) * mine + s], qg.at[n, s, 1], qg_send, qg_recv.at[s], sib).start()
    for s in range(mine):
        for n in range(2):
            kvb[(s * 2 + n) * cp + core] = kvown[core * mine + s, n]

    def wide(tab):
        return jnp.broadcast_to(tab[:, None, :], (blk, heads, head)).reshape(rows, head)

    def prepare(s, h, cos_q, sin_q):
        x = qg[0, s, h].astype(F32)
        rq[s, h * rows:(h + 1) * rows, :] = (x * cos_q + pltpu.roll(x, half_dim, 1) * sin_q).astype(BF16)
        put(g_t.at[s], h * rows, qg[1, s, h].T)

    def tables(h):
        cos_b, sin_b = tabs[h, 0], tabs[h, 1]
        put(tab_t, h * rows, wide(jnp.where(lane < half_dim, cos_b, sin_b) * scale).T)
        return wide(cos_b), wide(sin_b)

    put(diff, 0, lax.broadcasted_iota(jnp.int32, (blk, rows), 0) - lax.div(
        lax.broadcasted_iota(jnp.int32, (blk, rows), 1), heads))
    wait_bytes(qg.at[0], loc_sem)
    cs = tables(0)
    prepare(0, 0, *cs)
    kv_wave(0, 1)
    for s in range(1, mine):
        prepare(s, 0, *cs)
    tab_copy.wait_recv()
    cs = tables(1)
    for s in range(mine):
        wait_bytes(qg.at[0, 0], qg_recv.at[s])
        prepare(s, 1, *cs)
        if s + 1 < mine:
            kv_wave(s + 1, 0)
    for s in range(1, mine):
        kv_wave(s, 1)

    origin = chips - 2
    middle = origin - 1

    def send_far(s, x, d):
        base = (s * 2 + x) * cp
        slot = (core * mine + s) * 2 + x
        for k2 in range(CORES):
            remote(part.at[base + d * CORES + k2], rbuf.at[d * seqs * 2 + slot], r_sem.at[0], r_sem.at[1],
                   (chip - d) * CORES + k2).start()

    def send_near(s, x):
        base = (s * 2 + x) * cp
        slot = (core * mine + s) * 2 + x
        remote(part.at[base + 1 - core], rbuf.at[slot], r_sem.at[0], r_sem.at[1], sib).start()
        rbuf[slot] = part[base + core]

    def send_part(s, x, last):
        if last:
            for d in (chips - 1, *range(1, chips - 1)):
                send_far(s, x, d)
            send_near(s, x)
            return
        base = (s * 2 + x) * cp
        relayed = s == 0 and x in RELAYED
        for d in range(chips - 2, 0, -1):
            direct = chip >= d
            if relayed and d == origin:
                direct = None

                @pl.when(chip == origin)
                def _():
                    n = RELAYED.index(x) * CORES
                    for k2 in range(CORES):
                        remote(part.at[base + d * CORES + k2], passing.at[n + k2], r_sem.at[0], pass_sem,
                               middle * CORES + core).start()
            if relayed and d == middle:
                direct = jnp.logical_and(direct, chip != middle)
            if direct is not None:
                @pl.when(direct)
                def _():
                    send_far(s, x, d)
        send_near(s, x)

    def out_copy(src, dst, s):
        return remote(src.at[s], dst.at[core * mine + s], od_sem.at[0], od_sem.at[1], sib)

    def scores(s, first_slot, slots, row0):
        kk = kvb[s * 2 * cp + first_slot:s * 2 * cp + first_slot + slots].reshape(slots * blk, head)
        x = dot_nt(kk, rq[s, row0:row0 + ROWS, :])
        h, r = row0 // rows, row0 % rows
        owner = core if h == 0 else 1 - core
        dif = get(diff, r, ROWS)
        pieces = []
        for k in range(slots):
            xk = x[k * blk:(k + 1) * blk]
            if first_slot + k < CORES:
                xk = jnp.where(dif <= (owner - k) * blk, xk, -jnp.inf)
            else:
                xk = xk + jnp.where((first_slot + k) // CORES <= chip, 0.0, -jnp.inf)
            pieces.append(xk)
        return jnp.concatenate(pieces, axis=0)

    def pipeline(slots, last):
        n_keys = slots * blk
        near = 2 * CORES
        for s in range(mine):
            kv_wait(s, 0, last)
            if s == 0:
                for row0 in range(0, CORES * rows, ROWS):
                    put(x_s, row0, scores(s, 0, near, row0))
                far_wait(last)
            for row0 in range(0, CORES * rows, ROWS):
                if s == 0:
                    x = jnp.concatenate([get(x_s, row0, ROWS), scores(s, near, slots - near, row0)], axis=0)
                else:
                    x = scores(s, 0, slots, row0)
                mx = jnp.max(x, axis=0, keepdims=True)
                w = jnp.exp2((x - mx) * (scale * LOG2E))
                inv_l = 1.0 / jnp.sum(w, axis=0, keepdims=True)
                put(w_t, row0, w.astype(BF16))
                p = w * inv_l
                put(p_f, row0, p)
                put(p_t, row0, p.astype(BF16))
                norm[:, row0:row0 + ROWS] = inv_l
            at = (s * 2 + 1) * cp
            part[at:at + slots] = dot_nn(get(p_t, 0, CORES * rows, n_keys),
                                         qg[1, s].reshape(CORES * rows, head)).reshape(slots, blk, head)
            send_part(s, 1, last)
            kv_wait(s, 1, last)
            vv = kvb[at:at + slots].reshape(n_keys, head)
            v_t = vv.T
            for row0 in range(0, CORES * rows, ROWS):
                ot = (dot_nn(v_t, get(w_t, row0, ROWS, n_keys)) * norm[:, row0:row0 + ROWS]).astype(BF16)
                put(o_t.at[s], row0, ot)
                delta = jnp.sum(get(g_t.at[s], row0, ROWS).astype(F32) * ot.astype(F32), axis=0, keepdims=True)
                dp = dot_nt(vv, qg[1, s, row0 // rows, row0 % rows:row0 % rows + ROWS, :])
                put(ds_t.at[s], row0, (get(p_f, row0, ROWS, n_keys) * (dp - delta)).astype(BF16))
            at = s * 2 * cp
            part[at:at + slots] = dot_nn(get(ds_t.at[s], 0, CORES * rows, n_keys), rq[s]).reshape(slots, blk, head)
            send_part(s, 0, last)
    @pl.when(chip == chips - 1)
    def _():
        pipeline(cp, True)

    @pl.when(chip < chips - 1)
    def _():
        pipeline(cp - CORES, False)

    @pl.when(chip == middle)
    def _():
        wait_bytes(passing, pass_sem)
        for n, x in enumerate(RELAYED):
            first_slot = x * cp + middle * CORES
            part[first_slot:first_slot + CORES] += passing[n * CORES:(n + 1) * CORES]
            send_far(0, x, middle)

    for s in range(mine):
        k_t = kvb[s * 2 * cp:(s * 2 + 1) * cp].reshape(keys, head).T
        for h in (1, 0):
            for r in range(0, rows, ROWS):
                row0 = h * rows + r
                dq_t = dot_nn(k_t, get(ds_t.at[s], row0, ROWS))
                tab = get(tab_t, row0, ROWS)
                cos_q, sin_q = tab[:half_dim], tab[half_dim:]
                top, low = dq_t[:half_dim], dq_t[half_dim:]
                dq = jnp.concatenate([top * cos_q + low * sin_q, low * cos_q - top * sin_q], axis=0).astype(BF16).T
                out = get(o_t.at[s], row0, ROWS).T
                if h == 0:
                    dq_ref[core * mine + s, r:r + ROWS, :] = dq
                    o_ref[core * mine + s, r:r + ROWS, :] = out
                else:
                    dqsib[s, r:r + ROWS, :] = dq
                    osib[s, r:r + ROWS, :] = out
            if h == 1:
                out_copy(osib, o_ref, s).start()
                out_copy(dqsib, dq_ref, s).start()

    tab_copy.wait_send()
    wait_bytes(qg.at[0], qg_send)
    wait_by_chip(kvb, kv_send, lambda c: 2 * mine * (CORES * (chips - 1 - c) + 1))
    wait_bytes(qg.at[0], od_sem.at[0])
    wait_bytes(qg.at[0], od_sem.at[1])
    wait_by_chip(part, r_sem.at[0], lambda c: 2 * mine * (CORES * c + 1))
    wait_by_chip(rbuf, r_sem.at[1], lambda c: 2 * mine * (CORES * (chips - 1 - c) + 1)
                 - (CORES * len(RELAYED) if c == 0 else 0))


def finish_kernel(o_in, dq_in, rbuf, tabs, o_hbm, dq_hbm, dk_hbm, dv_hbm, dk_buf, dv_buf, sem):
    copies = [pltpu.make_async_copy(o_in, o_hbm, sem.at[0]), pltpu.make_async_copy(dq_in, dq_hbm, sem.at[1]),
              pltpu.make_async_copy(dk_buf, dk_hbm, sem.at[2]), pltpu.make_async_copy(dv_buf, dv_hbm, sem.at[3])]
    for c in copies[:2]:
        c.start()
    head = tabs.shape[-1]
    scale = head ** -0.5
    cos_t, sin_t = tabs[0], tabs[1]
    seqs = dk_buf.shape[0]
    for b in range(seqs):
        dk = rbuf[2 * b]
        dv = rbuf[2 * b + 1]
        for c in range(2 * seqs, rbuf.shape[0], 2 * seqs):
            dk = dk + rbuf[c + 2 * b]
            dv = dv + rbuf[c + 2 * b + 1]
        dk = dk * scale
        dk_buf[b] = (dk * cos_t - pltpu.roll(dk, head // 2, 1) * sin_t).astype(BF16)
        dv_buf[b] = dv.astype(BF16)
    for c in copies[2:]:
        c.start()
    for c in copies:
        c.wait()


def solution(mesh):
    cp = mesh.shape["cp"]
    query_spec = P("dp", "cp", None, None)
    kv_spec = P("dp", "cp", None)
    pos_spec = P(("dp", "cp"))

    def per_device(query, key, value, positions, grad_out):
        seqs, blk, heads, head = query.shape
        rows = blk * heads
        chips = cp // CORES
        mine = seqs // CORES
        keys = cp * blk
        tiles = CORES * rows // LANES
        freq = np.power(float(ROPE_BASE), -2.0 * np.arange(head // 2) / head)
        freq = jnp.asarray(np.concatenate([freq, freq])[None, :].astype(np.float32))
        vmem = pl.BlockSpec(memory_space=pltpu.VMEM)
        hbm = pl.BlockSpec(memory_space=pltpu.HBM)
        dma = pltpu.SemaphoreType.DMA
        big = jax.ShapeDtypeStruct((seqs, rows, head), BF16)
        small = jax.ShapeDtypeStruct((seqs, blk, head), BF16)
        o_mid, dq_mid, rbuf, tabs = pl.pallas_call(
            functools.partial(attend_kernel, cp, blk),
            out_shape=[big, big, jax.ShapeDtypeStruct((chips * seqs * 2, blk, head), F32),
                       jax.ShapeDtypeStruct((2, blk, head), F32)],
            in_specs=[hbm] * 6,
            out_specs=[vmem, vmem, vmem, vmem],
            scratch_shapes=[
                pltpu.VMEM((2, seqs, blk, head), BF16),
                pltpu.VMEM((1, blk), jnp.int32),
                pltpu.VMEM((1, head), F32),
                pltpu.VMEM((2, mine, CORES, rows, head), BF16),
                pltpu.VMEM((mine, CORES * rows, head), BF16),
                pltpu.VMEM((CORES, 2, blk, head), F32),
                pltpu.VMEM((seqs, 2, blk, head), BF16),
                pltpu.VMEM((mine * 2 * cp, blk, head), BF16),
                pltpu.VMEM((mine, tiles, head, LANES), BF16),
                pltpu.VMEM((tiles, head, LANES), F32),
                pltpu.VMEM((tiles, blk, LANES), jnp.int32),
                pltpu.VMEM((tiles, 2 * CORES * blk, LANES), F32),
                pltpu.VMEM((tiles, keys, LANES), BF16),
                pltpu.VMEM((tiles, keys, LANES), F32),
                pltpu.VMEM((1, CORES * rows), F32),
                pltpu.VMEM((tiles, keys, LANES), BF16),
                pltpu.VMEM((mine, tiles, keys, LANES), BF16),
                pltpu.VMEM((mine, tiles, head, LANES), BF16),
                pltpu.VMEM((mine * 2 * cp, blk, head), F32),
                pltpu.VMEM((CORES * len(RELAYED), blk, head), F32),
                pltpu.VMEM((mine, rows, head), BF16),
                pltpu.VMEM((mine, rows, head), BF16),
                dma((3,)), dma, dma, dma((mine,)), dma((2,)), dma, dma((mine, 2)), dma, dma((2,)), dma, dma((2,)),
            ],
            compiler_params=pltpu.CompilerParams(collective_id=0, has_side_effects=True,
                                                 vmem_limit_bytes=32 * 2 ** 20),
            name="attend",
        )(*(pltpu.with_memory_space_constraint(a, pltpu.HBM) for a in (
            query.reshape(seqs, rows, head), grad_out.reshape(seqs, rows, head), key, value,
            positions.reshape(1, blk), freq)))
        attn, dquery, dkey, dvalue = pl.pallas_call(
            finish_kernel,
            out_shape=[big, big, small, small],
            in_specs=[vmem] * 4,
            out_specs=[hbm] * 4,
            scratch_shapes=[pltpu.VMEM((seqs, blk, head), BF16), pltpu.VMEM((seqs, blk, head), BF16), dma((4,))],
            compiler_params=pltpu.CompilerParams(vmem_limit_bytes=16 * 2 ** 20),
            name="finish",
        )(o_mid, dq_mid, rbuf, tabs)
        shape = (seqs, blk, heads, head)
        return attn.reshape(shape), dquery.reshape(shape), dkey, dvalue

    return jax.shard_map(per_device, mesh=mesh, in_specs=(query_spec, kv_spec, kv_spec, pos_spec, query_spec),
                         out_specs=(query_spec, query_spec, kv_spec, kv_spec), check_vma=False)
```

```python
import functools

import jax
import jax.numpy as jnp
import numpy as np
from jax import lax
from jax.experimental import pallas as pl
from jax.experimental.pallas import tpu as pltpu
from jax.sharding import PartitionSpec as P

ROPE_BASE = 10000
CORES = 2
LOG2E = 1.4426950408889634
F32 = jnp.float32
BF16 = jnp.bfloat16
ROWS = 512
LANES = 128
RELAYED = (0,)


def dot_nn(a, b):
    return jnp.dot(a, b, preferred_element_type=F32)


def dot_nt(a, b):
    return lax.dot_general(a, b, (((1,), (1,)), ((), ())), preferred_element_type=F32)


def put(ref, row0, val):
    for n in range(0, val.shape[1], LANES):
        ref[(row0 + n) // LANES, :val.shape[0]] = val[:, n:n + LANES]


def get(ref, row0, count, height=None):
    height = ref.shape[1] if height is None else height
    return jnp.concatenate([ref[(row0 + n) // LANES, :height] for n in range(0, count, LANES)], axis=1)


def attend_kernel(cp, blk, q_hbm, g_hbm, k_hbm, v_hbm, pos_hbm, freq_hbm,
                  o_ref, dq_ref, rbuf, tabs_out,
                  kv_in, pos_ref, freq_ref, qg, rq, tabs, kvown, kvb, g_t, tab_t, diff,
                  w_s, run_max, w_t, p_f, norm, p_t, ds_t, o_t, part, passing, osib, dqsib,
                  first_sem, loc_sem, qg_send, qg_recv, tab_sem, kv_send, kv_recv, far_recv,
                  r_sem, pass_sem, od_sem):
    chips = cp // CORES
    seqs = q_hbm.shape[0]
    mine = seqs // CORES
    rows, head = q_hbm.shape[1], q_hbm.shape[2]
    heads = rows // blk
    half_dim = head // 2
    keys = cp * blk
    scale = head ** -0.5
    me = lax.axis_index("cp")
    chip = lax.div(me, CORES)
    core = lax.rem(me, CORES)
    sib = chip * CORES + 1 - core

    barrier = pltpu.get_barrier_semaphore()
    for d in range(1, cp):
        pl.semaphore_signal(barrier, inc=1, device_id={"cp": lax.rem(me + d, cp)},
                            device_id_type=pl.DeviceIdType.MESH)

    def remote(src, dst, ssem, rsem, dev):
        return pltpu.make_async_remote_copy(src_ref=src, dst_ref=dst, send_sem=ssem, recv_sem=rsem,
                                            device_id={"cp": dev}, device_id_type=pl.DeviceIdType.MESH)

    def wait_bytes(ref, sem):
        pltpu.make_async_copy(ref, ref, sem).wait()

    def wait_by_chip(ref, sem, blocks, last=None):
        if last:
            wait_bytes(ref.at[pl.ds(0, blocks(chips - 1))], sem)
            return
        for c in range(chips if last is None else chips - 1):
            if blocks(c):
                @pl.when(chip == c)
                def _():
                    wait_bytes(ref.at[pl.ds(0, blocks(c))], sem)

    first = [pltpu.make_async_copy(pos_hbm, pos_ref, first_sem.at[0]),
             pltpu.make_async_copy(freq_hbm, freq_ref, first_sem.at[1]),
             pltpu.make_async_copy(k_hbm, kv_in.at[0], first_sem.at[2]),
             pltpu.make_async_copy(v_hbm, kv_in.at[1], first_sem.at[2])]
    for c in first:
        c.start()
    for n, src in enumerate((q_hbm, g_hbm)):
        for s in range(mine):
            pltpu.make_async_copy(src.at[core * mine + s], qg.at[n, s, 0], loc_sem).start()

    for d in range(1, chips):
        @pl.when(d > chip)
        def _():
            for n in range(2 * mine):
                kvb[n * cp + d * CORES:n * cp + (d + 1) * CORES] = jnp.zeros((CORES, blk, head), BF16)

        if d == chips - 2:
            @pl.when(chip == 0)
            def _():
                for k2 in range(CORES):
                    for x in RELAYED:
                        rbuf[(d * seqs + k2 * mine) * 2 + x] = jnp.zeros((blk, head), F32)

        @pl.when(chip + d >= chips)
        def _():
            rbuf[d * seqs * 2:(d + 1) * seqs * 2] = jnp.zeros((seqs * 2, blk, head), F32)

    @pl.when(chip < chips - 1)
    def _():
        ds_t[:, :, keys - CORES * blk:] = jnp.zeros((mine, ds_t.shape[1], CORES * blk, LANES), BF16)

    first[0].wait()
    first[1].wait()
    pos_row = jnp.broadcast_to(pos_ref[...].astype(F32), (blk, blk))
    ident = lax.broadcasted_iota(jnp.int32, (blk, blk), 0) == lax.broadcasted_iota(jnp.int32, (blk, blk), 1)
    pos_col = jnp.sum(jnp.where(ident, pos_row, 0.0), axis=1, keepdims=True)
    ang = pos_col * freq_ref[...]
    cos_t = jnp.cos(ang)
    lane = lax.broadcasted_iota(jnp.int32, (blk, head), 1)
    sin_t = jnp.where(lane < half_dim, -jnp.sin(ang), jnp.sin(ang))
    tabs[0, 0] = cos_t
    tabs[0, 1] = sin_t
    tabs_out[0] = cos_t
    tabs_out[1] = sin_t
    wait_bytes(kv_in, first_sem.at[2])
    for b in range(seqs):
        kf = kv_in[0, b].astype(F32)
        kvown[b, 0] = (kf * cos_t + pltpu.roll(kf, half_dim, 1) * sin_t).astype(BF16)
        kvown[b, 1] = kv_in[1, b]

    pl.semaphore_wait(barrier, cp - 1)

    def kv_wave(s, n):
        base = (s * 2 + n) * cp
        for d in range(chips - 1, 0, -1):
            @pl.when(chip + d < chips)
            def _():
                for k2 in range(CORES):
                    remote(kvown.at[k2 * mine + s, n], kvb.at[base + d * CORES + core], kv_send,
                           far_recv if (s, n) == (0, 0) and d > 1 else kv_recv.at[s, n],
                           (chip + d) * CORES + k2).start()
        remote(kvown.at[(1 - core) * mine + s, n], kvb.at[base + core], kv_send, kv_recv.at[s, n], sib).start()

    def kv_wait(s, n, last):
        wait_by_chip(kvb, kv_recv.at[s, n], lambda c: CORES * (min(c, 1) if (s, n) == (0, 0) else c) + 1, last)

    def far_wait(last):
        wait_by_chip(kvb, far_recv, lambda c: CORES * max(c - 1, 0), last)

    tab_copy = remote(tabs.at[0], tabs.at[1], tab_sem.at[0], tab_sem.at[1], sib)

    kv_wave(0, 0)
    tab_copy.start()
    for s in range(mine):
        for n, src in enumerate((q_hbm, g_hbm)):
            remote(src.at[(1 - core) * mine + s], qg.at[n, s, 1], qg_send, qg_recv.at[s], sib).start()
    for s in range(mine):
        for n in range(2):
            kvb[(s * 2 + n) * cp + core] = kvown[core * mine + s, n]

    def wide(tab):
        return jnp.broadcast_to(tab[:, None, :], (blk, heads, head)).reshape(rows, head)

    def prepare(s, h, cos_q, sin_q):
        x = qg[0, s, h].astype(F32)
        rq[s, h * rows:(h + 1) * rows, :] = (x * cos_q + pltpu.roll(x, half_dim, 1) * sin_q).astype(BF16)
        put(g_t.at[s], h * rows, qg[1, s, h].T)

    def tables(h):
        cos_b, sin_b = tabs[h, 0], tabs[h, 1]
        put(tab_t, h * rows, wide(jnp.where(lane < half_dim, cos_b, sin_b) * scale).T)
        return wide(cos_b), wide(sin_b)

    put(diff, 0, lax.broadcasted_iota(jnp.int32, (blk, rows), 0) - lax.div(
        lax.broadcasted_iota(jnp.int32, (blk, rows), 1), heads))
    wait_bytes(qg.at[0], loc_sem)
    cs = tables(0)
    prepare(0, 0, *cs)
    kv_wave(0, 1)
    for s in range(1, mine):
        prepare(s, 0, *cs)
    tab_copy.wait_recv()
    cs = tables(1)
    for s in range(mine):
        wait_bytes(qg.at[0, 0], qg_recv.at[s])
        prepare(s, 1, *cs)
        if s + 1 < mine:
            kv_wave(s + 1, 0)
    for s in range(1, mine):
        kv_wave(s, 1)

    origin = chips - 2
    middle = origin - 1

    def send_far(s, x, d):
        base = (s * 2 + x) * cp
        slot = (core * mine + s) * 2 + x
        for k2 in range(CORES):
            remote(part.at[base + d * CORES + k2], rbuf.at[d * seqs * 2 + slot], r_sem.at[0], r_sem.at[1],
                   (chip - d) * CORES + k2).start()

    def send_near(s, x):
        base = (s * 2 + x) * cp
        slot = (core * mine + s) * 2 + x
        remote(part.at[base + 1 - core], rbuf.at[slot], r_sem.at[0], r_sem.at[1], sib).start()
        rbuf[slot] = part[base + core]

    def send_part(s, x, last):
        if last:
            for d in (chips - 1, *range(1, chips - 1)):
                send_far(s, x, d)
            send_near(s, x)
            return
        base = (s * 2 + x) * cp
        relayed = s == 0 and x in RELAYED
        for d in range(chips - 2, 0, -1):
            direct = chip >= d
            if relayed and d == origin:
                direct = None

                @pl.when(chip == origin)
                def _():
                    n = RELAYED.index(x) * CORES
                    for k2 in range(CORES):
                        remote(part.at[base + d * CORES + k2], passing.at[n + k2], r_sem.at[0], pass_sem,
                               middle * CORES + core).start()
            if relayed and d == middle:
                direct = jnp.logical_and(direct, chip != middle)
            if direct is not None:
                @pl.when(direct)
                def _():
                    send_far(s, x, d)
        send_near(s, x)

    def out_copy(src, dst, s):
        return remote(src.at[s], dst.at[core * mine + s], od_sem.at[0], od_sem.at[1], sib)

    def scores(s, first_slot, slots, row0):
        kk = kvb[s * 2 * cp + first_slot:s * 2 * cp + first_slot + slots].reshape(slots * blk, head)
        x = dot_nt(kk, rq[s, row0:row0 + ROWS, :])
        h, r = row0 // rows, row0 % rows
        owner = core if h == 0 else 1 - core
        dif = get(diff, r, ROWS)
        pieces = []
        for k in range(slots):
            xk = x[k * blk:(k + 1) * blk]
            if first_slot + k < CORES:
                xk = jnp.where(dif <= (owner - k) * blk, xk, -jnp.inf)
            else:
                xk = xk + jnp.where((first_slot + k) // CORES <= chip, 0.0, -jnp.inf)
            pieces.append(xk)
        return jnp.concatenate(pieces, axis=0)

    def pipeline(slots, last):
        n_keys = slots * blk
        near = 2 * CORES
        for s in range(mine):
            kv_wait(s, 0, last)
            if s == 0:
                for row0 in range(0, CORES * rows, ROWS):
                    x = scores(s, 0, near, row0)
                    mx = jnp.max(x, axis=0, keepdims=True)
                    w = jnp.exp2((x - mx) * (scale * LOG2E))
                    put(w_s, row0, w)
                    run_max[:, row0:row0 + ROWS] = mx
                    norm[:, row0:row0 + ROWS] = jnp.sum(w, axis=0, keepdims=True)
                far_wait(last)
            for row0 in range(0, CORES * rows, ROWS):
                if s == 0:
                    x = scores(s, near, slots - near, row0)
                    mx_near = run_max[:, row0:row0 + ROWS]
                    mx = jnp.maximum(mx_near, jnp.max(x, axis=0, keepdims=True))
                    factor = jnp.exp2((mx_near - mx) * (scale * LOG2E))
                    w = jnp.exp2((x - mx) * (scale * LOG2E))
                    inv_l = 1.0 / (norm[:, row0:row0 + ROWS] * factor + jnp.sum(w, axis=0, keepdims=True))
                    w = jnp.concatenate([get(w_s, row0, ROWS) * factor, w], axis=0)
                else:
                    x = scores(s, 0, slots, row0)
                    mx = jnp.max(x, axis=0, keepdims=True)
                    w = jnp.exp2((x - mx) * (scale * LOG2E))
                    inv_l = 1.0 / jnp.sum(w, axis=0, keepdims=True)
                put(w_t, row0, w.astype(BF16))
                p = w * inv_l
                put(p_f, row0, p)
                put(p_t, row0, p.astype(BF16))
                norm[:, row0:row0 + ROWS] = inv_l
            at = (s * 2 + 1) * cp
            part[at:at + slots] = dot_nn(get(p_t, 0, CORES * rows, n_keys),
                                         qg[1, s].reshape(CORES * rows, head)).reshape(slots, blk, head)
            send_part(s, 1, last)
            kv_wait(s, 1, last)
            vv = kvb[at:at + slots].reshape(n_keys, head)
            v_t = vv.T
            for row0 in range(0, CORES * rows, ROWS):
                ot = (dot_nn(v_t, get(w_t, row0, ROWS, n_keys)) * norm[:, row0:row0 + ROWS]).astype(BF16)
                put(o_t.at[s], row0, ot)
                delta = jnp.sum(get(g_t.at[s], row0, ROWS).astype(F32) * ot.astype(F32), axis=0, keepdims=True)
                dp = dot_nt(vv, qg[1, s, row0 // rows, row0 % rows:row0 % rows + ROWS, :])
                put(ds_t.at[s], row0, (get(p_f, row0, ROWS, n_keys) * (dp - delta)).astype(BF16))
            at = s * 2 * cp
            part[at:at + slots] = dot_nn(get(ds_t.at[s], 0, CORES * rows, n_keys), rq[s]).reshape(slots, blk, head)
            send_part(s, 0, last)
    @pl.when(chip == chips - 1)
    def _():
        pipeline(cp, True)

    @pl.when(chip < chips - 1)
    def _():
        pipeline(cp - CORES, False)

    @pl.when(chip == middle)
    def _():
        wait_bytes(passing, pass_sem)
        for n, x in enumerate(RELAYED):
            first_slot = x * cp + middle * CORES
            part[first_slot:first_slot + CORES] += passing[n * CORES:(n + 1) * CORES]
            send_far(0, x, middle)

    for s in range(mine):
        k_t = kvb[s * 2 * cp:(s * 2 + 1) * cp].reshape(keys, head).T
        for h in (1, 0):
            for r in range(0, rows, ROWS):
                row0 = h * rows + r
                dq_t = dot_nn(k_t, get(ds_t.at[s], row0, ROWS))
                tab = get(tab_t, row0, ROWS)
                cos_q, sin_q = tab[:half_dim], tab[half_dim:]
                top, low = dq_t[:half_dim], dq_t[half_dim:]
                dq = jnp.concatenate([top * cos_q + low * sin_q, low * cos_q - top * sin_q], axis=0).astype(BF16).T
                out = get(o_t.at[s], row0, ROWS).T
                if h == 0:
                    dq_ref[core * mine + s, r:r + ROWS, :] = dq
                    o_ref[core * mine + s, r:r + ROWS, :] = out
                else:
                    dqsib[s, r:r + ROWS, :] = dq
                    osib[s, r:r + ROWS, :] = out
            if h == 1:
                out_copy(osib, o_ref, s).start()
                out_copy(dqsib, dq_ref, s).start()

    tab_copy.wait_send()
    wait_bytes(qg.at[0], qg_send)
    wait_by_chip(kvb, kv_send, lambda c: 2 * mine * (CORES * (chips - 1 - c) + 1))
    wait_bytes(qg.at[0], od_sem.at[0])
    wait_bytes(qg.at[0], od_sem.at[1])
    wait_by_chip(part, r_sem.at[0], lambda c: 2 * mine * (CORES * c + 1))
    wait_by_chip(rbuf, r_sem.at[1], lambda c: 2 * mine * (CORES * (chips - 1 - c) + 1)
                 - (CORES * len(RELAYED) if c == 0 else 0))


def finish_kernel(o_in, dq_in, rbuf, tabs, o_hbm, dq_hbm, dk_hbm, dv_hbm, dk_buf, dv_buf, sem):
    copies = [pltpu.make_async_copy(o_in, o_hbm, sem.at[0]), pltpu.make_async_copy(dq_in, dq_hbm, sem.at[1]),
              pltpu.make_async_copy(dk_buf, dk_hbm, sem.at[2]), pltpu.make_async_copy(dv_buf, dv_hbm, sem.at[3])]
    for c in copies[:2]:
        c.start()
    head = tabs.shape[-1]
    scale = head ** -0.5
    cos_t, sin_t = tabs[0], tabs[1]
    seqs = dk_buf.shape[0]
    for b in range(seqs):
        dk = rbuf[2 * b]
        dv = rbuf[2 * b + 1]
        for c in range(2 * seqs, rbuf.shape[0], 2 * seqs):
            dk = dk + rbuf[c + 2 * b]
            dv = dv + rbuf[c + 2 * b + 1]
        dk = dk * scale
        dk_buf[b] = (dk * cos_t - pltpu.roll(dk, head // 2, 1) * sin_t).astype(BF16)
        dv_buf[b] = dv.astype(BF16)
    for c in copies[2:]:
        c.start()
    for c in copies:
        c.wait()


def solution(mesh):
    cp = mesh.shape["cp"]
    query_spec = P("dp", "cp", None, None)
    kv_spec = P("dp", "cp", None)
    pos_spec = P(("dp", "cp"))

    def per_device(query, key, value, positions, grad_out):
        seqs, blk, heads, head = query.shape
        rows = blk * heads
        chips = cp // CORES
        mine = seqs // CORES
        keys = cp * blk
        tiles = CORES * rows // LANES
        freq = np.power(float(ROPE_BASE), -2.0 * np.arange(head // 2) / head)
        freq = jnp.asarray(np.concatenate([freq, freq])[None, :].astype(np.float32))
        vmem = pl.BlockSpec(memory_space=pltpu.VMEM)
        hbm = pl.BlockSpec(memory_space=pltpu.HBM)
        dma = pltpu.SemaphoreType.DMA
        big = jax.ShapeDtypeStruct((seqs, rows, head), BF16)
        small = jax.ShapeDtypeStruct((seqs, blk, head), BF16)
        o_mid, dq_mid, rbuf, tabs = pl.pallas_call(
            functools.partial(attend_kernel, cp, blk),
            out_shape=[big, big, jax.ShapeDtypeStruct((chips * seqs * 2, blk, head), F32),
                       jax.ShapeDtypeStruct((2, blk, head), F32)],
            in_specs=[hbm] * 6,
            out_specs=[vmem, vmem, vmem, vmem],
            scratch_shapes=[
                pltpu.VMEM((2, seqs, blk, head), BF16),
                pltpu.VMEM((1, blk), jnp.int32),
                pltpu.VMEM((1, head), F32),
                pltpu.VMEM((2, mine, CORES, rows, head), BF16),
                pltpu.VMEM((mine, CORES * rows, head), BF16),
                pltpu.VMEM((CORES, 2, blk, head), F32),
                pltpu.VMEM((seqs, 2, blk, head), BF16),
                pltpu.VMEM((mine * 2 * cp, blk, head), BF16),
                pltpu.VMEM((mine, tiles, head, LANES), BF16),
                pltpu.VMEM((tiles, head, LANES), F32),
                pltpu.VMEM((tiles, blk, LANES), jnp.int32),
                pltpu.VMEM((tiles, 2 * CORES * blk, LANES), F32),
                pltpu.VMEM((1, CORES * rows), F32),
                pltpu.VMEM((tiles, keys, LANES), BF16),
                pltpu.VMEM((tiles, keys, LANES), F32),
                pltpu.VMEM((1, CORES * rows), F32),
                pltpu.VMEM((tiles, keys, LANES), BF16),
                pltpu.VMEM((mine, tiles, keys, LANES), BF16),
                pltpu.VMEM((mine, tiles, head, LANES), BF16),
                pltpu.VMEM((mine * 2 * cp, blk, head), F32),
                pltpu.VMEM((CORES * len(RELAYED), blk, head), F32),
                pltpu.VMEM((mine, rows, head), BF16),
                pltpu.VMEM((mine, rows, head), BF16),
                dma((3,)), dma, dma, dma((mine,)), dma((2,)), dma, dma((mine, 2)), dma, dma((2,)), dma, dma((2,)),
            ],
            compiler_params=pltpu.CompilerParams(collective_id=0, has_side_effects=True,
                                                 vmem_limit_bytes=32 * 2 ** 20),
            name="attend",
        )(*(pltpu.with_memory_space_constraint(a, pltpu.HBM) for a in (
            query.reshape(seqs, rows, head), grad_out.reshape(seqs, rows, head), key, value,
            positions.reshape(1, blk), freq)))
        attn, dquery, dkey, dvalue = pl.pallas_call(
            finish_kernel,
            out_shape=[big, big, small, small],
            in_specs=[vmem] * 4,
            out_specs=[hbm] * 4,
            scratch_shapes=[pltpu.VMEM((seqs, blk, head), BF16), pltpu.VMEM((seqs, blk, head), BF16), dma((4,))],
            compiler_params=pltpu.CompilerParams(vmem_limit_bytes=16 * 2 ** 20),
            name="finish",
        )(o_mid, dq_mid, rbuf, tabs)
        shape = (seqs, blk, heads, head)
        return attn.reshape(shape), dquery.reshape(shape), dkey, dvalue

    return jax.shard_map(per_device, mesh=mesh, in_specs=(query_spec, kv_spec, kv_spec, pos_spec, query_spec),
                         out_specs=(query_spec, query_spec, kv_spec, kv_spec), check_vma=False)
```

```python
import functools

import jax
import jax.numpy as jnp
import numpy as np
from jax import lax
from jax.experimental import pallas as pl
from jax.experimental.pallas import tpu as pltpu
from jax.sharding import PartitionSpec as P

ROPE_BASE = 10000
CORES = 2
LOG2E = 1.4426950408889634
F32 = jnp.float32
BF16 = jnp.bfloat16
ROWS = 512
LANES = 128
RELAYED = (0,)


def dot_nn(a, b):
    return jnp.dot(a, b, preferred_element_type=F32)


def dot_nt(a, b):
    return lax.dot_general(a, b, (((1,), (1,)), ((), ())), preferred_element_type=F32)


def put(ref, row0, val):
    for n in range(0, val.shape[1], LANES):
        ref[(row0 + n) // LANES, :val.shape[0]] = val[:, n:n + LANES]


def get(ref, row0, count, height=None):
    height = ref.shape[1] if height is None else height
    return jnp.concatenate([ref[(row0 + n) // LANES, :height] for n in range(0, count, LANES)], axis=1)


def attend_kernel(cp, blk, q_hbm, g_hbm, k_hbm, v_hbm, pos_hbm, freq_hbm,
                  o_ref, dq_ref, rbuf, tabs_out,
                  kv_in, pos_ref, freq_ref, qg, rq, tabs, kvown, kvb, g_t, tab_t, diff,
                  w_s, run_max, w_t, p_f, norm, p_t, ds_t, o_t, part, passing, osib, dqsib,
                  first_sem, loc_sem, qg_send, qg_recv, tab_sem, kv_send, kv_recv, far_recv,
                  r_sem, pass_sem, od_sem):
    chips = cp // CORES
    seqs = q_hbm.shape[0]
    mine = seqs // CORES
    rows, head = q_hbm.shape[1], q_hbm.shape[2]
    heads = rows // blk
    half_dim = head // 2
    keys = cp * blk
    scale = head ** -0.5
    me = lax.axis_index("cp")
    chip = lax.div(me, CORES)
    core = lax.rem(me, CORES)
    sib = chip * CORES + 1 - core

    barrier = pltpu.get_barrier_semaphore()
    for d in range(1, cp):
        pl.semaphore_signal(barrier, inc=1, device_id={"cp": lax.rem(me + d, cp)},
                            device_id_type=pl.DeviceIdType.MESH)

    def remote(src, dst, ssem, rsem, dev):
        return pltpu.make_async_remote_copy(src_ref=src, dst_ref=dst, send_sem=ssem, recv_sem=rsem,
                                            device_id={"cp": dev}, device_id_type=pl.DeviceIdType.MESH)

    def wait_bytes(ref, sem):
        pltpu.make_async_copy(ref, ref, sem).wait()

    def wait_by_chip(ref, sem, blocks, last=None):
        if last:
            wait_bytes(ref.at[pl.ds(0, blocks(chips - 1))], sem)
            return
        for c in range(chips if last is None else chips - 1):
            if blocks(c):
                @pl.when(chip == c)
                def _():
                    wait_bytes(ref.at[pl.ds(0, blocks(c))], sem)

    first = [pltpu.make_async_copy(pos_hbm, pos_ref, first_sem.at[0]),
             pltpu.make_async_copy(freq_hbm, freq_ref, first_sem.at[1]),
             pltpu.make_async_copy(k_hbm, kv_in.at[0], first_sem.at[2]),
             pltpu.make_async_copy(v_hbm, kv_in.at[1], first_sem.at[2])]
    for c in first:
        c.start()
    for n, src in enumerate((q_hbm, g_hbm)):
        for s in range(mine):
            pltpu.make_async_copy(src.at[core * mine + s], qg.at[n, s, 0], loc_sem).start()

    for d in range(1, chips):
        @pl.when(d > chip)
        def _():
            for n in range(2 * mine):
                kvb[n * cp + d * CORES:n * cp + (d + 1) * CORES] = jnp.zeros((CORES, blk, head), BF16)

        if d == chips - 2:
            @pl.when(chip == 0)
            def _():
                for k2 in range(CORES):
                    for x in RELAYED:
                        rbuf[(d * seqs + k2 * mine) * 2 + x] = jnp.zeros((blk, head), F32)

        @pl.when(chip + d >= chips)
        def _():
            rbuf[d * seqs * 2:(d + 1) * seqs * 2] = jnp.zeros((seqs * 2, blk, head), F32)

    @pl.when(chip < chips - 1)
    def _():
        ds_t[:, :, keys - CORES * blk:] = jnp.zeros((mine, ds_t.shape[1], CORES * blk, LANES), BF16)

    first[0].wait()
    first[1].wait()
    pos_row = jnp.broadcast_to(pos_ref[...].astype(F32), (blk, blk))
    ident = lax.broadcasted_iota(jnp.int32, (blk, blk), 0) == lax.broadcasted_iota(jnp.int32, (blk, blk), 1)
    pos_col = jnp.sum(jnp.where(ident, pos_row, 0.0), axis=1, keepdims=True)
    ang = pos_col * freq_ref[...]
    cos_t = jnp.cos(ang)
    lane = lax.broadcasted_iota(jnp.int32, (blk, head), 1)
    sin_t = jnp.where(lane < half_dim, -jnp.sin(ang), jnp.sin(ang))
    tabs[0, 0] = cos_t
    tabs[0, 1] = sin_t
    tabs_out[0] = cos_t
    tabs_out[1] = sin_t
    wait_bytes(kv_in, first_sem.at[2])
    for b in range(seqs):
        kf = kv_in[0, b].astype(F32)
        kvown[b, 0] = (kf * cos_t + pltpu.roll(kf, half_dim, 1) * sin_t).astype(BF16)
        kvown[b, 1] = kv_in[1, b]

    pl.semaphore_wait(barrier, cp - 1)

    def kv_wave(s, n):
        base = (s * 2 + n) * cp
        for d in range(chips - 1, 0, -1):
            @pl.when(chip + d < chips)
            def _():
                for k2 in range(CORES):
                    remote(kvown.at[k2 * mine + s, n], kvb.at[base + d * CORES + core], kv_send,
                           far_recv if (s, n) == (0, 0) and d > 1 else kv_recv.at[s, n],
                           (chip + d) * CORES + k2).start()
        remote(kvown.at[(1 - core) * mine + s, n], kvb.at[base + core], kv_send, kv_recv.at[s, n], sib).start()

    def kv_wait(s, n, last):
        wait_by_chip(kvb, kv_recv.at[s, n], lambda c: CORES * (min(c, 1) if (s, n) == (0, 0) else c) + 1, last)

    def far_wait(last):
        wait_by_chip(kvb, far_recv, lambda c: CORES * max(c - 1, 0), last)

    tab_copy = remote(tabs.at[0], tabs.at[1], tab_sem.at[0], tab_sem.at[1], sib)

    kv_wave(0, 0)
    tab_copy.start()
    for s in range(mine):
        for n, src in enumerate((q_hbm, g_hbm)):
            remote(src.at[(1 - core) * mine + s], qg.at[n, s, 1], qg_send, qg_recv.at[s], sib).start()
    for s in range(mine):
        for n in range(2):
            kvb[(s * 2 + n) * cp + core] = kvown[core * mine + s, n]

    def wide(tab):
        return jnp.broadcast_to(tab[:, None, :], (blk, heads, head)).reshape(rows, head)

    def prepare(s, h, cos_q, sin_q):
        x = qg[0, s, h].astype(F32)
        rq[s, h * rows:(h + 1) * rows, :] = (x * cos_q + pltpu.roll(x, half_dim, 1) * sin_q).astype(BF16)
        put(g_t.at[s], h * rows, qg[1, s, h].T)

    def tables(h):
        cos_b, sin_b = tabs[h, 0], tabs[h, 1]
        put(tab_t, h * rows, wide(jnp.where(lane < half_dim, cos_b, sin_b) * scale).T)
        return wide(cos_b), wide(sin_b)

    put(diff, 0, lax.broadcasted_iota(jnp.int32, (blk, rows), 0) - lax.div(
        lax.broadcasted_iota(jnp.int32, (blk, rows), 1), heads))
    wait_bytes(qg.at[0], loc_sem)
    cs = tables(0)
    prepare(0, 0, *cs)
    kv_wave(0, 1)
    for s in range(1, mine):
        prepare(s, 0, *cs)
    tab_copy.wait_recv()
    cs = tables(1)
    for s in range(mine):
        if s + 1 < mine:
            kv_wave(s + 1, 0)
        wait_bytes(qg.at[0, 0], qg_recv.at[s])
        prepare(s, 1, *cs)
        if s + 1 < mine:
            kv_wave(s + 1, 1)

    origin = chips - 2
    middle = origin - 1

    def send_far(s, x, d):
        base = (s * 2 + x) * cp
        slot = (core * mine + s) * 2 + x
        for k2 in range(CORES):
            remote(part.at[base + d * CORES + k2], rbuf.at[d * seqs * 2 + slot], r_sem.at[0], r_sem.at[1],
                   (chip - d) * CORES + k2).start()

    def send_near(s, x):
        base = (s * 2 + x) * cp
        slot = (core * mine + s) * 2 + x
        remote(part.at[base + 1 - core], rbuf.at[slot], r_sem.at[0], r_sem.at[1], sib).start()
        rbuf[slot] = part[base + core]

    def send_part(s, x, last):
        if last:
            for d in (chips - 1, *range(1, chips - 1)):
                send_far(s, x, d)
            send_near(s, x)
            return
        base = (s * 2 + x) * cp
        relayed = s == 0 and x in RELAYED
        for d in range(chips - 2, 0, -1):
            direct = chip >= d
            if relayed and d == origin:
                direct = None

                @pl.when(chip == origin)
                def _():
                    n = RELAYED.index(x) * CORES
                    for k2 in range(CORES):
                        remote(part.at[base + d * CORES + k2], passing.at[n + k2], r_sem.at[0], pass_sem,
                               middle * CORES + core).start()
            if relayed and d == middle:
                direct = jnp.logical_and(direct, chip != middle)
            if direct is not None:
                @pl.when(direct)
                def _():
                    send_far(s, x, d)
        send_near(s, x)

    def out_copy(src, dst, s):
        return remote(src.at[s], dst.at[core * mine + s], od_sem.at[0], od_sem.at[1], sib)

    def scores(s, first_slot, slots, row0, last):
        kk = kvb[s * 2 * cp + first_slot:s * 2 * cp + first_slot + slots].reshape(slots * blk, head)
        x = dot_nt(kk, rq[s, row0:row0 + ROWS, :])
        h, r = row0 // rows, row0 % rows
        owner = core if h == 0 else 1 - core
        dif = get(diff, r, ROWS)
        pieces = []
        for k in range(slots):
            xk = x[k * blk:(k + 1) * blk]
            if first_slot + k < CORES:
                xk = jnp.where(dif <= (owner - k) * blk, xk, -jnp.inf)
            elif not last:
                xk = xk + jnp.where((first_slot + k) // CORES <= chip, 0.0, -jnp.inf)
            pieces.append(xk)
        return jnp.concatenate(pieces, axis=0)

    def pipeline(slots, last):
        n_keys = slots * blk
        near = 2 * CORES
        for s in range(mine):
            kv_wait(s, 0, last)
            if s == 0:
                for row0 in range(0, CORES * rows, ROWS):
                    x = scores(s, 0, near, row0, last)
                    mx = jnp.max(x, axis=0, keepdims=True)
                    w = jnp.exp2((x - mx) * (scale * LOG2E))
                    put(w_s, row0, w)
                    run_max[:, row0:row0 + ROWS] = mx
                    norm[:, row0:row0 + ROWS] = jnp.sum(w, axis=0, keepdims=True)
                far_wait(last)
            for row0 in range(0, CORES * rows, ROWS):
                if s == 0:
                    x = scores(s, near, slots - near, row0, last)
                    mx_near = run_max[:, row0:row0 + ROWS]
                    mx = jnp.maximum(mx_near, jnp.max(x, axis=0, keepdims=True))
                    factor = jnp.exp2((mx_near - mx) * (scale * LOG2E))
                    w = jnp.exp2((x - mx) * (scale * LOG2E))
                    inv_l = 1.0 / (norm[:, row0:row0 + ROWS] * factor + jnp.sum(w, axis=0, keepdims=True))
                    w = jnp.concatenate([get(w_s, row0, ROWS) * factor, w], axis=0)
                else:
                    x = scores(s, 0, slots, row0, last)
                    mx = jnp.max(x, axis=0, keepdims=True)
                    w = jnp.exp2((x - mx) * (scale * LOG2E))
                    inv_l = 1.0 / jnp.sum(w, axis=0, keepdims=True)
                put(w_t, row0, w.astype(BF16))
                p = w * inv_l
                put(p_f, row0, p)
                put(p_t, row0, p.astype(BF16))
                norm[:, row0:row0 + ROWS] = inv_l
            at = (s * 2 + 1) * cp
            part[at:at + slots] = dot_nn(get(p_t, 0, CORES * rows, n_keys),
                                         qg[1, s].reshape(CORES * rows, head)).reshape(slots, blk, head)
            send_part(s, 1, last)
            kv_wait(s, 1, last)
            vv = kvb[at:at + slots].reshape(n_keys, head)
            v_t = vv.T
            for row0 in range(0, CORES * rows, ROWS):
                ot = (dot_nn(v_t, get(w_t, row0, ROWS, n_keys)) * norm[:, row0:row0 + ROWS]).astype(BF16)
                put(o_t.at[s], row0, ot)
                delta = jnp.sum(get(g_t.at[s], row0, ROWS).astype(F32) * ot.astype(F32), axis=0, keepdims=True)
                dp = dot_nt(vv, qg[1, s, row0 // rows, row0 % rows:row0 % rows + ROWS, :])
                put(ds_t.at[s], row0, (get(p_f, row0, ROWS, n_keys) * (dp - delta)).astype(BF16))
            at = s * 2 * cp
            part[at:at + slots] = dot_nn(get(ds_t.at[s], 0, CORES * rows, n_keys), rq[s]).reshape(slots, blk, head)
            send_part(s, 0, last)
    @pl.when(chip == chips - 1)
    def _():
        pipeline(cp, True)

    @pl.when(chip < chips - 1)
    def _():
        pipeline(cp - CORES, False)

    @pl.when(chip == middle)
    def _():
        wait_bytes(passing, pass_sem)
        for n, x in enumerate(RELAYED):
            first_slot = x * cp + middle * CORES
            part[first_slot:first_slot + CORES] += passing[n * CORES:(n + 1) * CORES]
            send_far(0, x, middle)

    for s in range(mine):
        k_t = kvb[s * 2 * cp:(s * 2 + 1) * cp].reshape(keys, head).T
        for h in (1, 0):
            for r in range(0, rows, ROWS):
                row0 = h * rows + r
                dq_t = dot_nn(k_t, get(ds_t.at[s], row0, ROWS))
                tab = get(tab_t, row0, ROWS)
                cos_q, sin_q = tab[:half_dim], tab[half_dim:]
                top, low = dq_t[:half_dim], dq_t[half_dim:]
                dq = jnp.concatenate([top * cos_q + low * sin_q, low * cos_q - top * sin_q], axis=0).astype(BF16).T
                out = get(o_t.at[s], row0, ROWS).T
                if h == 0:
                    dq_ref[core * mine + s, r:r + ROWS, :] = dq
                    o_ref[core * mine + s, r:r + ROWS, :] = out
                else:
                    dqsib[s, r:r + ROWS, :] = dq
                    osib[s, r:r + ROWS, :] = out
            if h == 1:
                out_copy(osib, o_ref, s).start()
                out_copy(dqsib, dq_ref, s).start()

    tab_copy.wait_send()
    wait_bytes(qg.at[0], qg_send)
    wait_by_chip(kvb, kv_send, lambda c: 2 * mine * (CORES * (chips - 1 - c) + 1))
    wait_bytes(qg.at[0], od_sem.at[0])
    wait_bytes(qg.at[0], od_sem.at[1])
    wait_by_chip(part, r_sem.at[0], lambda c: 2 * mine * (CORES * c + 1))
    wait_by_chip(rbuf, r_sem.at[1], lambda c: 2 * mine * (CORES * (chips - 1 - c) + 1)
                 - (CORES * len(RELAYED) if c == 0 else 0))


def finish_kernel(o_in, dq_in, rbuf, tabs, o_hbm, dq_hbm, dk_hbm, dv_hbm, dk_buf, dv_buf, sem):
    copies = [pltpu.make_async_copy(o_in, o_hbm, sem.at[0]), pltpu.make_async_copy(dq_in, dq_hbm, sem.at[1]),
              pltpu.make_async_copy(dk_buf, dk_hbm, sem.at[2]), pltpu.make_async_copy(dv_buf, dv_hbm, sem.at[3])]
    for c in copies[:2]:
        c.start()
    head = tabs.shape[-1]
    scale = head ** -0.5
    cos_t, sin_t = tabs[0], tabs[1]
    seqs = dk_buf.shape[0]
    for b in range(seqs):
        dk = rbuf[2 * b]
        dv = rbuf[2 * b + 1]
        for c in range(2 * seqs, rbuf.shape[0], 2 * seqs):
            dk = dk + rbuf[c + 2 * b]
            dv = dv + rbuf[c + 2 * b + 1]
        dk = dk * scale
        dk_buf[b] = (dk * cos_t - pltpu.roll(dk, head // 2, 1) * sin_t).astype(BF16)
        dv_buf[b] = dv.astype(BF16)
    for c in copies[2:]:
        c.start()
    for c in copies:
        c.wait()


def solution(mesh):
    cp = mesh.shape["cp"]
    query_spec = P("dp", "cp", None, None)
    kv_spec = P("dp", "cp", None)
    pos_spec = P(("dp", "cp"))

    def per_device(query, key, value, positions, grad_out):
        seqs, blk, heads, head = query.shape
        rows = blk * heads
        chips = cp // CORES
        mine = seqs // CORES
        keys = cp * blk
        tiles = CORES * rows // LANES
        freq = np.power(float(ROPE_BASE), -2.0 * np.arange(head // 2) / head)
        freq = jnp.asarray(np.concatenate([freq, freq])[None, :].astype(np.float32))
        vmem = pl.BlockSpec(memory_space=pltpu.VMEM)
        hbm = pl.BlockSpec(memory_space=pltpu.HBM)
        dma = pltpu.SemaphoreType.DMA
        big = jax.ShapeDtypeStruct((seqs, rows, head), BF16)
        small = jax.ShapeDtypeStruct((seqs, blk, head), BF16)
        o_mid, dq_mid, rbuf, tabs = pl.pallas_call(
            functools.partial(attend_kernel, cp, blk),
            out_shape=[big, big, jax.ShapeDtypeStruct((chips * seqs * 2, blk, head), F32),
                       jax.ShapeDtypeStruct((2, blk, head), F32)],
            in_specs=[hbm] * 6,
            out_specs=[vmem, vmem, vmem, vmem],
            scratch_shapes=[
                pltpu.VMEM((2, seqs, blk, head), BF16),
                pltpu.VMEM((1, blk), jnp.int32),
                pltpu.VMEM((1, head), F32),
                pltpu.VMEM((2, mine, CORES, rows, head), BF16),
                pltpu.VMEM((mine, CORES * rows, head), BF16),
                pltpu.VMEM((CORES, 2, blk, head), F32),
                pltpu.VMEM((seqs, 2, blk, head), BF16),
                pltpu.VMEM((mine * 2 * cp, blk, head), BF16),
                pltpu.VMEM((mine, tiles, head, LANES), BF16),
                pltpu.VMEM((tiles, head, LANES), F32),
                pltpu.VMEM((tiles, blk, LANES), jnp.int32),
                pltpu.VMEM((tiles, 2 * CORES * blk, LANES), F32),
                pltpu.VMEM((1, CORES * rows), F32),
                pltpu.VMEM((tiles, keys, LANES), BF16),
                pltpu.VMEM((tiles, keys, LANES), F32),
                pltpu.VMEM((1, CORES * rows), F32),
                pltpu.VMEM((tiles, keys, LANES), BF16),
                pltpu.VMEM((mine, tiles, keys, LANES), BF16),
                pltpu.VMEM((mine, tiles, head, LANES), BF16),
                pltpu.VMEM((mine * 2 * cp, blk, head), F32),
                pltpu.VMEM((CORES * len(RELAYED), blk, head), F32),
                pltpu.VMEM((mine, rows, head), BF16),
                pltpu.VMEM((mine, rows, head), BF16),
                dma((3,)), dma, dma, dma((mine,)), dma((2,)), dma, dma((mine, 2)), dma, dma((2,)), dma, dma((2,)),
            ],
            compiler_params=pltpu.CompilerParams(collective_id=0, has_side_effects=True,
                                                 vmem_limit_bytes=32 * 2 ** 20),
            name="attend",
        )(*(pltpu.with_memory_space_constraint(a, pltpu.HBM) for a in (
            query.reshape(seqs, rows, head), grad_out.reshape(seqs, rows, head), key, value,
            positions.reshape(1, blk), freq)))
        attn, dquery, dkey, dvalue = pl.pallas_call(
            finish_kernel,
            out_shape=[big, big, small, small],
            in_specs=[vmem] * 4,
            out_specs=[hbm] * 4,
            scratch_shapes=[pltpu.VMEM((seqs, blk, head), BF16), pltpu.VMEM((seqs, blk, head), BF16), dma((4,))],
            compiler_params=pltpu.CompilerParams(vmem_limit_bytes=16 * 2 ** 20),
            name="finish",
        )(o_mid, dq_mid, rbuf, tabs)
        shape = (seqs, blk, heads, head)
        return attn.reshape(shape), dquery.reshape(shape), dkey, dvalue

    return jax.shard_map(per_device, mesh=mesh, in_specs=(query_spec, kv_spec, kv_spec, pos_spec, query_spec),
                         out_specs=(query_spec, query_spec, kv_spec, kv_spec), check_vma=False)
```

```python
import functools

import jax
import jax.numpy as jnp
import numpy as np
from jax import lax
from jax.experimental import pallas as pl
from jax.experimental.pallas import tpu as pltpu
from jax.sharding import PartitionSpec as P

ROPE_BASE = 10000
CORES = 2
LOG2E = 1.4426950408889634
F32 = jnp.float32
BF16 = jnp.bfloat16
ROWS = 512
LANES = 128
RELAYED = (0,)


def dot_nn(a, b):
    return jnp.dot(a, b, preferred_element_type=F32)


def dot_nt(a, b):
    return lax.dot_general(a, b, (((1,), (1,)), ((), ())), preferred_element_type=F32)


def put(ref, row0, val):
    for n in range(0, val.shape[1], LANES):
        ref[(row0 + n) // LANES, :val.shape[0]] = val[:, n:n + LANES]


def get(ref, row0, count, height=None):
    height = ref.shape[1] if height is None else height
    return jnp.concatenate([ref[(row0 + n) // LANES, :height] for n in range(0, count, LANES)], axis=1)


def attend_kernel(cp, blk, q_hbm, g_hbm, k_hbm, v_hbm, pos_hbm, freq_hbm,
                  o_ref, dq_ref, rbuf, tabs_out,
                  kv_in, pos_ref, freq_ref, qg, rq, tabs, kvown, kvb, g_t, tab_t, diff,
                  w_s, run_max, w_t, p_f, norm, p_t, ds_t, o_t, part, passing, osib, dqsib,
                  first_sem, loc_sem, qg_send, qg_recv, tab_sem, kv_send, kv_recv, far_recv,
                  r_sem, pass_sem, od_sem):
    chips = cp // CORES
    seqs = q_hbm.shape[0]
    mine = seqs // CORES
    rows, head = q_hbm.shape[1], q_hbm.shape[2]
    heads = rows // blk
    half_dim = head // 2
    keys = cp * blk
    scale = head ** -0.5
    me = lax.axis_index("cp")
    chip = lax.div(me, CORES)
    core = lax.rem(me, CORES)
    sib = chip * CORES + 1 - core

    barrier = pltpu.get_barrier_semaphore()
    for d in range(1, cp):
        pl.semaphore_signal(barrier, inc=1, device_id={"cp": lax.rem(me + d, cp)},
                            device_id_type=pl.DeviceIdType.MESH)

    def remote(src, dst, ssem, rsem, dev):
        return pltpu.make_async_remote_copy(src_ref=src, dst_ref=dst, send_sem=ssem, recv_sem=rsem,
                                            device_id={"cp": dev}, device_id_type=pl.DeviceIdType.MESH)

    def wait_bytes(ref, sem):
        pltpu.make_async_copy(ref, ref, sem).wait()

    def wait_by_chip(ref, sem, blocks, last=None):
        if last:
            wait_bytes(ref.at[pl.ds(0, blocks(chips - 1))], sem)
            return
        for c in range(chips if last is None else chips - 1):
            if blocks(c):
                @pl.when(chip == c)
                def _():
                    wait_bytes(ref.at[pl.ds(0, blocks(c))], sem)

    first = [pltpu.make_async_copy(pos_hbm, pos_ref, first_sem.at[0]),
             pltpu.make_async_copy(freq_hbm, freq_ref, first_sem.at[1]),
             pltpu.make_async_copy(k_hbm, kv_in.at[0], first_sem.at[2]),
             pltpu.make_async_copy(v_hbm, kv_in.at[1], first_sem.at[2])]
    for c in first:
        c.start()
    for n, src in enumerate((q_hbm, g_hbm)):
        for s in range(mine):
            pltpu.make_async_copy(src.at[core * mine + s], qg.at[n, s, 0], loc_sem).start()

    for d in range(1, chips):
        @pl.when(d > chip)
        def _():
            for n in range(2 * mine):
                kvb[n * cp + d * CORES:n * cp + (d + 1) * CORES] = jnp.zeros((CORES, blk, head), BF16)

        if d == chips - 2:
            @pl.when(chip == 0)
            def _():
                for k2 in range(CORES):
                    for x in RELAYED:
                        rbuf[(d * seqs + k2 * mine) * 2 + x] = jnp.zeros((blk, head), F32)

        @pl.when(chip + d >= chips)
        def _():
            rbuf[d * seqs * 2:(d + 1) * seqs * 2] = jnp.zeros((seqs * 2, blk, head), F32)

    @pl.when(chip < chips - 1)
    def _():
        ds_t[:, :, keys - CORES * blk:] = jnp.zeros((mine, ds_t.shape[1], CORES * blk, LANES), BF16)

    first[0].wait()
    first[1].wait()
    pos_row = jnp.broadcast_to(pos_ref[...].astype(F32), (blk, blk))
    ident = lax.broadcasted_iota(jnp.int32, (blk, blk), 0) == lax.broadcasted_iota(jnp.int32, (blk, blk), 1)
    pos_col = jnp.sum(jnp.where(ident, pos_row, 0.0), axis=1, keepdims=True)
    ang = pos_col * freq_ref[...]
    cos_t = jnp.cos(ang)
    lane = lax.broadcasted_iota(jnp.int32, (blk, head), 1)
    sin_t = jnp.where(lane < half_dim, -jnp.sin(ang), jnp.sin(ang))
    tabs[0, 0] = cos_t
    tabs[0, 1] = sin_t
    tabs_out[0] = cos_t
    tabs_out[1] = sin_t
    wait_bytes(kv_in, first_sem.at[2])
    for b in range(seqs):
        kf = kv_in[0, b].astype(F32)
        kvown[b, 0] = (kf * cos_t + pltpu.roll(kf, half_dim, 1) * sin_t).astype(BF16)
        kvown[b, 1] = kv_in[1, b]

    pl.semaphore_wait(barrier, cp - 1)

    def kv_wave(s, n):
        base = (s * 2 + n) * cp
        for d in range(chips - 1, 0, -1):
            @pl.when(chip + d < chips)
            def _():
                for k2 in range(CORES):
                    remote(kvown.at[k2 * mine + s, n], kvb.at[base + d * CORES + core], kv_send,
                           far_recv if (s, n) == (0, 0) and d > 1 else kv_recv.at[s, n],
                           (chip + d) * CORES + k2).start()
        remote(kvown.at[(1 - core) * mine + s, n], kvb.at[base + core], kv_send, kv_recv.at[s, n], sib).start()

    def kv_wait(s, n, last):
        wait_by_chip(kvb, kv_recv.at[s, n], lambda c: CORES * (min(c, 1) if (s, n) == (0, 0) else c) + 1, last)

    def far_wait(last):
        wait_by_chip(kvb, far_recv, lambda c: CORES * max(c - 1, 0), last)

    tab_copy = remote(tabs.at[0], tabs.at[1], tab_sem.at[0], tab_sem.at[1], sib)

    kv_wave(0, 0)
    tab_copy.start()
    for s in range(mine):
        for n, src in enumerate((q_hbm, g_hbm)):
            remote(src.at[(1 - core) * mine + s], qg.at[n, s, 1], qg_send, qg_recv.at[s], sib).start()
    for s in range(mine):
        for n in range(2):
            kvb[(s * 2 + n) * cp + core] = kvown[core * mine + s, n]

    def wide(tab):
        return jnp.broadcast_to(tab[:, None, :], (blk, heads, head)).reshape(rows, head)

    def prepare(s, h, cos_q, sin_q):
        x = qg[0, s, h].astype(F32)
        rq[s, h * rows:(h + 1) * rows, :] = (x * cos_q + pltpu.roll(x, half_dim, 1) * sin_q).astype(BF16)
        put(g_t.at[s], h * rows, qg[1, s, h].T)

    def tables(h):
        cos_b, sin_b = tabs[h, 0], tabs[h, 1]
        put(tab_t, h * rows, wide(jnp.where(lane < half_dim, cos_b, sin_b) * scale).T)
        return wide(cos_b), wide(sin_b)

    put(diff, 0, lax.broadcasted_iota(jnp.int32, (blk, rows), 0) - lax.div(
        lax.broadcasted_iota(jnp.int32, (blk, rows), 1), heads))
    wait_bytes(qg.at[0], loc_sem)
    cs = tables(0)
    prepare(0, 0, *cs)
    kv_wave(0, 1)
    for s in range(1, mine):
        prepare(s, 0, *cs)
    tab_copy.wait_recv()
    cs = tables(1)
    for s in range(mine):
        if s + 1 < mine:
            kv_wave(s + 1, 0)
        wait_bytes(qg.at[0, 0], qg_recv.at[s])
        prepare(s, 1, *cs)
        if s + 1 < mine:
            kv_wave(s + 1, 1)

    origin = chips - 2
    middle = origin - 1

    def send_far(s, x, d):
        base = (s * 2 + x) * cp
        slot = (core * mine + s) * 2 + x
        for k2 in reversed(range(CORES)):
            remote(part.at[base + d * CORES + k2], rbuf.at[d * seqs * 2 + slot], r_sem.at[0], r_sem.at[1],
                   (chip - d) * CORES + k2).start()

    def send_near(s, x):
        base = (s * 2 + x) * cp
        slot = (core * mine + s) * 2 + x
        remote(part.at[base + 1 - core], rbuf.at[slot], r_sem.at[0], r_sem.at[1], sib).start()
        rbuf[slot] = part[base + core]

    def send_part(s, x, last):
        if last:
            for d in (chips - 1, *range(1, chips - 1)):
                send_far(s, x, d)
            send_near(s, x)
            return
        base = (s * 2 + x) * cp
        relayed = s == 0 and x in RELAYED
        for d in range(chips - 2, 0, -1):
            direct = chip >= d
            if relayed and d == origin:
                direct = None

                @pl.when(chip == origin)
                def _():
                    n = RELAYED.index(x) * CORES
                    for k2 in range(CORES):
                        remote(part.at[base + d * CORES + k2], passing.at[n + k2], r_sem.at[0], pass_sem,
                               middle * CORES + core).start()
            if relayed and d == middle:
                direct = jnp.logical_and(direct, chip != middle)
            if s == 0 and d == 1:
                direct = jnp.logical_and(direct, chip != origin)
            if direct is not None:
                @pl.when(direct)
                def _():
                    send_far(s, x, d)
        send_near(s, x)
        if (s, x) == (1, 1):
            @pl.when(chip == origin)
            def _():
                for late in (1, 0):
                    send_far(0, late, 1)

    def out_copy(src, dst, s):
        return remote(src.at[s], dst.at[core * mine + s], od_sem.at[0], od_sem.at[1], sib)

    def scores(s, first_slot, slots, row0, last):
        kk = kvb[s * 2 * cp + first_slot:s * 2 * cp + first_slot + slots].reshape(slots * blk, head)
        x = dot_nt(kk, rq[s, row0:row0 + ROWS, :])
        h, r = row0 // rows, row0 % rows
        owner = core if h == 0 else 1 - core
        dif = get(diff, r, ROWS)
        pieces = []
        for k in range(slots):
            xk = x[k * blk:(k + 1) * blk]
            if first_slot + k < CORES:
                xk = jnp.where(dif <= (owner - k) * blk, xk, -jnp.inf)
            elif not last:
                xk = xk + jnp.where((first_slot + k) // CORES <= chip, 0.0, -jnp.inf)
            pieces.append(xk)
        return jnp.concatenate(pieces, axis=0)

    def pipeline(slots, last):
        n_keys = slots * blk
        near = 2 * CORES
        for s in range(mine):
            kv_wait(s, 0, last)
            if s == 0:
                for row0 in range(0, CORES * rows, ROWS):
                    x = scores(s, 0, near, row0, last)
                    mx = jnp.max(x, axis=0, keepdims=True)
                    w = jnp.exp2((x - mx) * (scale * LOG2E))
                    put(w_s, row0, w)
                    run_max[:, row0:row0 + ROWS] = mx
                    norm[:, row0:row0 + ROWS] = jnp.sum(w, axis=0, keepdims=True)
                far_wait(last)
            for row0 in range(0, CORES * rows, ROWS):
                if s == 0:
                    x = scores(s, near, slots - near, row0, last)
                    mx_near = run_max[:, row0:row0 + ROWS]
                    mx = jnp.maximum(mx_near, jnp.max(x, axis=0, keepdims=True))
                    factor = jnp.exp2((mx_near - mx) * (scale * LOG2E))
                    w = jnp.exp2((x - mx) * (scale * LOG2E))
                    inv_l = 1.0 / (norm[:, row0:row0 + ROWS] * factor + jnp.sum(w, axis=0, keepdims=True))
                    w = jnp.concatenate([get(w_s, row0, ROWS) * factor, w], axis=0)
                else:
                    x = scores(s, 0, slots, row0, last)
                    mx = jnp.max(x, axis=0, keepdims=True)
                    w = jnp.exp2((x - mx) * (scale * LOG2E))
                    inv_l = 1.0 / jnp.sum(w, axis=0, keepdims=True)
                put(w_t, row0, w.astype(BF16))
                p = w * inv_l
                put(p_f, row0, p)
                put(p_t, row0, p.astype(BF16))
                norm[:, row0:row0 + ROWS] = inv_l
            at = (s * 2 + 1) * cp
            part[at:at + slots] = dot_nn(get(p_t, 0, CORES * rows, n_keys),
                                         qg[1, s].reshape(CORES * rows, head)).reshape(slots, blk, head)
            send_part(s, 1, last)
            kv_wait(s, 1, last)
            vv = kvb[at:at + slots].reshape(n_keys, head)
            v_t = vv.T
            for row0 in range(0, CORES * rows, ROWS):
                ot = (dot_nn(v_t, get(w_t, row0, ROWS, n_keys)) * norm[:, row0:row0 + ROWS]).astype(BF16)
                put(o_t.at[s], row0, ot)
                delta = jnp.sum(get(g_t.at[s], row0, ROWS).astype(F32) * ot.astype(F32), axis=0, keepdims=True)
                dp = dot_nt(vv, qg[1, s, row0 // rows, row0 % rows:row0 % rows + ROWS, :])
                put(ds_t.at[s], row0, (get(p_f, row0, ROWS, n_keys) * (dp - delta)).astype(BF16))
            at = s * 2 * cp
            part[at:at + slots] = dot_nn(get(ds_t.at[s], 0, CORES * rows, n_keys), rq[s]).reshape(slots, blk, head)
            send_part(s, 0, last)
    @pl.when(chip == chips - 1)
    def _():
        pipeline(cp, True)

    @pl.when(chip < chips - 1)
    def _():
        pipeline(cp - CORES, False)

    @pl.when(chip == middle)
    def _():
        wait_bytes(passing, pass_sem)
        for n, x in enumerate(RELAYED):
            first_slot = x * cp + middle * CORES
            part[first_slot:first_slot + CORES] += passing[n * CORES:(n + 1) * CORES]
            send_far(0, x, middle)

    for s in range(mine):
        k_t = kvb[s * 2 * cp:(s * 2 + 1) * cp].reshape(keys, head).T
        for h in (1, 0):
            for r in range(0, rows, ROWS):
                row0 = h * rows + r
                dq_t = dot_nn(k_t, get(ds_t.at[s], row0, ROWS))
                tab = get(tab_t, row0, ROWS)
                cos_q, sin_q = tab[:half_dim], tab[half_dim:]
                top, low = dq_t[:half_dim], dq_t[half_dim:]
                dq = jnp.concatenate([top * cos_q + low * sin_q, low * cos_q - top * sin_q], axis=0).astype(BF16).T
                out = get(o_t.at[s], row0, ROWS).T
                if h == 0:
                    dq_ref[core * mine + s, r:r + ROWS, :] = dq
                    o_ref[core * mine + s, r:r + ROWS, :] = out
                else:
                    dqsib[s, r:r + ROWS, :] = dq
                    osib[s, r:r + ROWS, :] = out
            if h == 1:
                out_copy(osib, o_ref, s).start()
                out_copy(dqsib, dq_ref, s).start()

    tab_copy.wait_send()
    wait_bytes(qg.at[0], qg_send)
    wait_by_chip(kvb, kv_send, lambda c: 2 * mine * (CORES * (chips - 1 - c) + 1))
    wait_bytes(qg.at[0], od_sem.at[0])
    wait_bytes(qg.at[0], od_sem.at[1])
    wait_by_chip(part, r_sem.at[0], lambda c: 2 * mine * (CORES * c + 1))
    wait_by_chip(rbuf, r_sem.at[1], lambda c: 2 * mine * (CORES * (chips - 1 - c) + 1)
                 - (CORES * len(RELAYED) if c == 0 else 0))


def finish_kernel(o_in, dq_in, rbuf, tabs, o_hbm, dq_hbm, dk_hbm, dv_hbm, dk_buf, dv_buf, sem):
    copies = [pltpu.make_async_copy(o_in, o_hbm, sem.at[0]), pltpu.make_async_copy(dq_in, dq_hbm, sem.at[1]),
              pltpu.make_async_copy(dk_buf, dk_hbm, sem.at[2]), pltpu.make_async_copy(dv_buf, dv_hbm, sem.at[3])]
    for c in copies[:2]:
        c.start()
    head = tabs.shape[-1]
    scale = head ** -0.5
    cos_t, sin_t = tabs[0], tabs[1]
    seqs = dk_buf.shape[0]
    for b in range(seqs):
        dk = rbuf[2 * b]
        dv = rbuf[2 * b + 1]
        for c in range(2 * seqs, rbuf.shape[0], 2 * seqs):
            dk = dk + rbuf[c + 2 * b]
            dv = dv + rbuf[c + 2 * b + 1]
        dk = dk * scale
        dk_buf[b] = (dk * cos_t - pltpu.roll(dk, head // 2, 1) * sin_t).astype(BF16)
        dv_buf[b] = dv.astype(BF16)
    for c in copies[2:]:
        c.start()
    for c in copies:
        c.wait()


def solution(mesh):
    cp = mesh.shape["cp"]
    query_spec = P("dp", "cp", None, None)
    kv_spec = P("dp", "cp", None)
    pos_spec = P(("dp", "cp"))

    def per_device(query, key, value, positions, grad_out):
        seqs, blk, heads, head = query.shape
        rows = blk * heads
        chips = cp // CORES
        mine = seqs // CORES
        keys = cp * blk
        tiles = CORES * rows // LANES
        freq = np.power(float(ROPE_BASE), -2.0 * np.arange(head // 2) / head)
        freq = jnp.asarray(np.concatenate([freq, freq])[None, :].astype(np.float32))
        vmem = pl.BlockSpec(memory_space=pltpu.VMEM)
        hbm = pl.BlockSpec(memory_space=pltpu.HBM)
        dma = pltpu.SemaphoreType.DMA
        big = jax.ShapeDtypeStruct((seqs, rows, head), BF16)
        small = jax.ShapeDtypeStruct((seqs, blk, head), BF16)
        o_mid, dq_mid, rbuf, tabs = pl.pallas_call(
            functools.partial(attend_kernel, cp, blk),
            out_shape=[big, big, jax.ShapeDtypeStruct((chips * seqs * 2, blk, head), F32),
                       jax.ShapeDtypeStruct((2, blk, head), F32)],
            in_specs=[hbm] * 6,
            out_specs=[vmem, vmem, vmem, vmem],
            scratch_shapes=[
                pltpu.VMEM((2, seqs, blk, head), BF16),
                pltpu.VMEM((1, blk), jnp.int32),
                pltpu.VMEM((1, head), F32),
                pltpu.VMEM((2, mine, CORES, rows, head), BF16),
                pltpu.VMEM((mine, CORES * rows, head), BF16),
                pltpu.VMEM((CORES, 2, blk, head), F32),
                pltpu.VMEM((seqs, 2, blk, head), BF16),
                pltpu.VMEM((mine * 2 * cp, blk, head), BF16),
                pltpu.VMEM((mine, tiles, head, LANES), BF16),
                pltpu.VMEM((tiles, head, LANES), F32),
                pltpu.VMEM((tiles, blk, LANES), jnp.int32),
                pltpu.VMEM((tiles, 2 * CORES * blk, LANES), F32),
                pltpu.VMEM((1, CORES * rows), F32),
                pltpu.VMEM((tiles, keys, LANES), BF16),
                pltpu.VMEM((tiles, keys, LANES), F32),
                pltpu.VMEM((1, CORES * rows), F32),
                pltpu.VMEM((tiles, keys, LANES), BF16),
                pltpu.VMEM((mine, tiles, keys, LANES), BF16),
                pltpu.VMEM((mine, tiles, head, LANES), BF16),
                pltpu.VMEM((mine * 2 * cp, blk, head), F32),
                pltpu.VMEM((CORES * len(RELAYED), blk, head), F32),
                pltpu.VMEM((mine, rows, head), BF16),
                pltpu.VMEM((mine, rows, head), BF16),
                dma((3,)), dma, dma, dma((mine,)), dma((2,)), dma, dma((mine, 2)), dma, dma((2,)), dma, dma((2,)),
            ],
            compiler_params=pltpu.CompilerParams(collective_id=0, has_side_effects=True,
                                                 vmem_limit_bytes=32 * 2 ** 20),
            name="attend",
        )(*(pltpu.with_memory_space_constraint(a, pltpu.HBM) for a in (
            query.reshape(seqs, rows, head), grad_out.reshape(seqs, rows, head), key, value,
            positions.reshape(1, blk), freq)))
        attn, dquery, dkey, dvalue = pl.pallas_call(
            finish_kernel,
            out_shape=[big, big, small, small],
            in_specs=[vmem] * 4,
            out_specs=[hbm] * 4,
            scratch_shapes=[pltpu.VMEM((seqs, blk, head), BF16), pltpu.VMEM((seqs, blk, head), BF16), dma((4,))],
            compiler_params=pltpu.CompilerParams(vmem_limit_bytes=16 * 2 ** 20),
            name="finish",
        )(o_mid, dq_mid, rbuf, tabs)
        shape = (seqs, blk, heads, head)
        return attn.reshape(shape), dquery.reshape(shape), dkey, dvalue

    return jax.shard_map(per_device, mesh=mesh, in_specs=(query_spec, kv_spec, kv_spec, pos_spec, query_spec),
                         out_specs=(query_spec, query_spec, kv_spec, kv_spec), check_vma=False)
```

```python
import functools

import jax
import jax.numpy as jnp
import numpy as np
from jax import lax
from jax.experimental import pallas as pl
from jax.experimental.pallas import tpu as pltpu
from jax.sharding import PartitionSpec as P

ROPE_BASE = 10000
CORES = 2
LOG2E = 1.4426950408889634
F32 = jnp.float32
BF16 = jnp.bfloat16
ROWS = 512
LANES = 128
RELAYED = (0,)


def dot_nn(a, b):
    return jnp.dot(a, b, preferred_element_type=F32)


def dot_nt(a, b):
    return lax.dot_general(a, b, (((1,), (1,)), ((), ())), preferred_element_type=F32)


def put(ref, row0, val):
    for n in range(0, val.shape[1], LANES):
        ref[(row0 + n) // LANES, :val.shape[0]] = val[:, n:n + LANES]


def get(ref, row0, count, height=None):
    height = ref.shape[1] if height is None else height
    return jnp.concatenate([ref[(row0 + n) // LANES, :height] for n in range(0, count, LANES)], axis=1)


def attend_kernel(cp, blk, q_hbm, g_hbm, k_hbm, v_hbm, pos_hbm, freq_hbm,
                  o_ref, dq_ref, rbuf, tabs_out,
                  kv_in, pos_ref, freq_ref, qg, rq, tabs, kvown, kvb, g_t, tab_t, diff,
                  w_s, run_max, w_t, p_f, norm, p_t, ds_t, o_t, part, passing, osib, dqsib,
                  first_sem, loc_sem, qg_recv, tab_sem, kv_recv, far_recv,
                  r_sem, pass_sem, od_sem):
    chips = cp // CORES
    seqs = q_hbm.shape[0]
    mine = seqs // CORES
    rows, head = q_hbm.shape[1], q_hbm.shape[2]
    heads = rows // blk
    half_dim = head // 2
    keys = cp * blk
    scale = head ** -0.5
    me = lax.axis_index("cp")
    chip = lax.div(me, CORES)
    core = lax.rem(me, CORES)
    sib = chip * CORES + 1 - core

    barrier = pltpu.get_barrier_semaphore()
    for d in range(1, cp):
        pl.semaphore_signal(barrier, inc=1, device_id={"cp": lax.rem(me + d, cp)},
                            device_id_type=pl.DeviceIdType.MESH)

    def remote(src, dst, ssem, rsem, dev):
        return pltpu.make_async_remote_copy(src_ref=src, dst_ref=dst, send_sem=ssem, recv_sem=rsem,
                                            device_id={"cp": dev}, device_id_type=pl.DeviceIdType.MESH)

    def wait_bytes(ref, sem):
        pltpu.make_async_copy(ref, ref, sem).wait()

    def wait_by_chip(ref, sem, blocks, last=None):
        if last:
            wait_bytes(ref.at[pl.ds(0, blocks(chips - 1))], sem)
            return
        for c in range(chips if last is None else chips - 1):
            if blocks(c):
                @pl.when(chip == c)
                def _():
                    wait_bytes(ref.at[pl.ds(0, blocks(c))], sem)

    first = [pltpu.make_async_copy(pos_hbm, pos_ref, first_sem.at[0]),
             pltpu.make_async_copy(freq_hbm, freq_ref, first_sem.at[1]),
             pltpu.make_async_copy(k_hbm, kv_in.at[0], first_sem.at[2]),
             pltpu.make_async_copy(v_hbm, kv_in.at[1], first_sem.at[2])]
    for c in first:
        c.start()
    for n, src in enumerate((q_hbm, g_hbm)):
        for s in range(mine):
            pltpu.make_async_copy(src.at[core * mine + s], qg.at[n, s, 0], loc_sem).start()

    for d in range(1, chips):
        @pl.when(d > chip)
        def _():
            for n in range(2 * mine):
                kvb[n * cp + d * CORES:n * cp + (d + 1) * CORES] = jnp.zeros((CORES, blk, head), BF16)

        if d == chips - 2:
            @pl.when(chip == 0)
            def _():
                for k2 in range(CORES):
                    for x in RELAYED:
                        rbuf[(d * seqs + k2 * mine) * 2 + x] = jnp.zeros((blk, head), F32)

        @pl.when(chip + d >= chips)
        def _():
            rbuf[d * seqs * 2:(d + 1) * seqs * 2] = jnp.zeros((seqs * 2, blk, head), F32)

    @pl.when(chip < chips - 1)
    def _():
        ds_t[:, :, keys - CORES * blk:] = jnp.zeros((mine, ds_t.shape[1], CORES * blk, LANES), BF16)

    first[0].wait()
    first[1].wait()
    pos_row = jnp.broadcast_to(pos_ref[...].astype(F32), (blk, blk))
    ident = lax.broadcasted_iota(jnp.int32, (blk, blk), 0) == lax.broadcasted_iota(jnp.int32, (blk, blk), 1)
    pos_col = jnp.sum(jnp.where(ident, pos_row, 0.0), axis=1, keepdims=True)
    ang = pos_col * freq_ref[...]
    cos_t = jnp.cos(ang)
    lane = lax.broadcasted_iota(jnp.int32, (blk, head), 1)
    sin_t = jnp.where(lane < half_dim, -jnp.sin(ang), jnp.sin(ang))
    tabs[0, 0] = cos_t
    tabs[0, 1] = sin_t
    tabs_out[0] = cos_t
    tabs_out[1] = sin_t
    wait_bytes(kv_in, first_sem.at[2])
    for b in range(seqs):
        kf = kv_in[0, b].astype(F32)
        kvown[b, 0] = (kf * cos_t + pltpu.roll(kf, half_dim, 1) * sin_t).astype(BF16)
        kvown[b, 1] = kv_in[1, b]

    pl.semaphore_wait(barrier, cp - 1)

    def kv_wave(s, n):
        base = (s * 2 + n) * cp
        for d in range(chips - 1, 0, -1):
            @pl.when(chip + d < chips)
            def _():
                for k2 in range(CORES):
                    remote(kvown.at[k2 * mine + s, n], kvb.at[base + d * CORES + core], r_sem.at[0],
                           far_recv if (s, n) == (0, 0) and d > 1 else kv_recv.at[s, n],
                           (chip + d) * CORES + k2).start()
        remote(kvown.at[(1 - core) * mine + s, n], kvb.at[base + core], r_sem.at[0], kv_recv.at[s, n], sib).start()

    def kv_wait(s, n, last):
        wait_by_chip(kvb, kv_recv.at[s, n], lambda c: CORES * (min(c, 1) if (s, n) == (0, 0) else c) + 1, last)

    def far_wait(last):
        wait_by_chip(kvb, far_recv, lambda c: CORES * max(c - 1, 0), last)

    tab_copy = remote(tabs.at[0], tabs.at[1], r_sem.at[0], tab_sem, sib)

    kv_wave(0, 0)
    tab_copy.start()
    for s in range(mine):
        for n, src in enumerate((q_hbm, g_hbm)):
            remote(src.at[(1 - core) * mine + s], qg.at[n, s, 1], od_sem.at[0], qg_recv.at[s], sib).start()
    for s in range(mine):
        for n in range(2):
            kvb[(s * 2 + n) * cp + core] = kvown[core * mine + s, n]

    def wide(tab):
        return jnp.broadcast_to(tab[:, None, :], (blk, heads, head)).reshape(rows, head)

    def prepare(s, h, cos_q, sin_q):
        x = qg[0, s, h].astype(F32)
        rq[s, h * rows:(h + 1) * rows, :] = (x * cos_q + pltpu.roll(x, half_dim, 1) * sin_q).astype(BF16)
        put(g_t.at[s], h * rows, qg[1, s, h].T)

    def tables(h):
        cos_b, sin_b = tabs[h, 0], tabs[h, 1]
        put(tab_t, h * rows, wide(jnp.where(lane < half_dim, cos_b, sin_b) * scale).T)
        return wide(cos_b), wide(sin_b)

    put(diff, 0, lax.broadcasted_iota(jnp.int32, (blk, rows), 0) - lax.div(
        lax.broadcasted_iota(jnp.int32, (blk, rows), 1), heads))
    wait_bytes(qg.at[0], loc_sem)
    cs = tables(0)
    prepare(0, 0, *cs)
    kv_wave(0, 1)
    for s in range(1, mine):
        prepare(s, 0, *cs)
    tab_copy.wait_recv()
    cs = tables(1)
    for s in range(mine):
        if s + 1 < mine:
            kv_wave(s + 1, 0)
        wait_bytes(qg.at[0, 0], qg_recv.at[s])
        prepare(s, 1, *cs)
        if s + 1 < mine:
            kv_wave(s + 1, 1)

    origin = chips - 2
    middle = origin - 1

    def send_far(s, x, d):
        base = (s * 2 + x) * cp
        slot = (core * mine + s) * 2 + x
        for k2 in reversed(range(CORES)):
            remote(part.at[base + d * CORES + k2], rbuf.at[d * seqs * 2 + slot], r_sem.at[0], r_sem.at[1],
                   (chip - d) * CORES + k2).start()

    def send_near(s, x):
        base = (s * 2 + x) * cp
        slot = (core * mine + s) * 2 + x
        remote(part.at[base + 1 - core], rbuf.at[slot], r_sem.at[0], r_sem.at[1], sib).start()
        rbuf[slot] = part[base + core]

    def send_part(s, x, last):
        if last:
            for d in (chips - 1, *range(1, chips - 1)):
                send_far(s, x, d)
            send_near(s, x)
            return
        base = (s * 2 + x) * cp
        relayed = s == 0 and x in RELAYED
        for d in range(chips - 2, 0, -1):
            direct = chip >= d
            if relayed and d == origin:
                direct = None

                @pl.when(chip == origin)
                def _():
                    n = RELAYED.index(x) * CORES
                    for k2 in range(CORES):
                        remote(part.at[base + d * CORES + k2], passing.at[n + k2], r_sem.at[0], pass_sem,
                               middle * CORES + core).start()
            if relayed and d == middle:
                direct = jnp.logical_and(direct, chip != middle)
            if s == 0 and d == 1:
                direct = jnp.logical_and(direct, chip != origin)
            if direct is not None:
                @pl.when(direct)
                def _():
                    send_far(s, x, d)
        send_near(s, x)
        if (s, x) == (1, 1):
            @pl.when(chip == origin)
            def _():
                for late in (1, 0):
                    send_far(0, late, 1)

    def out_copy(src, dst, s):
        return remote(src.at[s], dst.at[core * mine + s], od_sem.at[0], od_sem.at[1], sib)

    def scores(s, first_slot, slots, row0, last):
        kk = kvb[s * 2 * cp + first_slot:s * 2 * cp + first_slot + slots].reshape(slots * blk, head)
        x = dot_nt(kk, rq[s, row0:row0 + ROWS, :])
        h, r = row0 // rows, row0 % rows
        owner = core if h == 0 else 1 - core
        dif = get(diff, r, ROWS)
        pieces = []
        for k in range(slots):
            xk = x[k * blk:(k + 1) * blk]
            if first_slot + k < CORES:
                xk = jnp.where(dif <= (owner - k) * blk, xk, -jnp.inf)
            elif not last:
                xk = xk + jnp.where((first_slot + k) // CORES <= chip, 0.0, -jnp.inf)
            pieces.append(xk)
        return jnp.concatenate(pieces, axis=0)

    def pipeline(slots, last):
        n_keys = slots * blk
        near = 2 * CORES
        for s in range(mine):
            kv_wait(s, 0, last)
            if s == 0:
                for row0 in range(0, CORES * rows, ROWS):
                    x = scores(s, 0, near, row0, last)
                    mx = jnp.max(x, axis=0, keepdims=True)
                    w = jnp.exp2((x - mx) * (scale * LOG2E))
                    put(w_s, row0, w)
                    run_max[:, row0:row0 + ROWS] = mx
                    norm[:, row0:row0 + ROWS] = jnp.sum(w, axis=0, keepdims=True)
                far_wait(last)
            for row0 in range(0, CORES * rows, ROWS):
                if s == 0:
                    x = scores(s, near, slots - near, row0, last)
                    mx_near = run_max[:, row0:row0 + ROWS]
                    mx = jnp.maximum(mx_near, jnp.max(x, axis=0, keepdims=True))
                    factor = jnp.exp2((mx_near - mx) * (scale * LOG2E))
                    w = jnp.exp2((x - mx) * (scale * LOG2E))
                    inv_l = 1.0 / (norm[:, row0:row0 + ROWS] * factor + jnp.sum(w, axis=0, keepdims=True))
                    w = jnp.concatenate([get(w_s, row0, ROWS) * factor, w], axis=0)
                else:
                    x = scores(s, 0, slots, row0, last)
                    mx = jnp.max(x, axis=0, keepdims=True)
                    w = jnp.exp2((x - mx) * (scale * LOG2E))
                    inv_l = 1.0 / jnp.sum(w, axis=0, keepdims=True)
                put(w_t, row0, w.astype(BF16))
                p = w * inv_l
                put(p_f, row0, p)
                put(p_t, row0, p.astype(BF16))
                norm[:, row0:row0 + ROWS] = inv_l
            at = (s * 2 + 1) * cp
            part[at:at + slots] = dot_nn(get(p_t, 0, CORES * rows, n_keys),
                                         qg[1, s].reshape(CORES * rows, head)).reshape(slots, blk, head)
            send_part(s, 1, last)
            kv_wait(s, 1, last)
            vv = kvb[at:at + slots].reshape(n_keys, head)
            v_t = vv.T
            for row0 in range(0, CORES * rows, ROWS):
                ot = (dot_nn(v_t, get(w_t, row0, ROWS, n_keys)) * norm[:, row0:row0 + ROWS]).astype(BF16)
                put(o_t.at[s], row0, ot)
                delta = jnp.sum(get(g_t.at[s], row0, ROWS).astype(F32) * ot.astype(F32), axis=0, keepdims=True)
                dp = dot_nt(vv, qg[1, s, row0 // rows, row0 % rows:row0 % rows + ROWS, :])
                put(ds_t.at[s], row0, (get(p_f, row0, ROWS, n_keys) * (dp - delta)).astype(BF16))
            at = s * 2 * cp
            part[at:at + slots] = dot_nn(get(ds_t.at[s], 0, CORES * rows, n_keys), rq[s]).reshape(slots, blk, head)
            send_part(s, 0, last)
    @pl.when(chip == chips - 1)
    def _():
        pipeline(cp, True)

    @pl.when(chip < chips - 1)
    def _():
        pipeline(cp - CORES, False)

    @pl.when(chip == middle)
    def _():
        wait_bytes(passing, pass_sem)
        for n, x in enumerate(RELAYED):
            first_slot = x * cp + middle * CORES
            part[first_slot:first_slot + CORES] += passing[n * CORES:(n + 1) * CORES]
            send_far(0, x, middle)

    for s in range(mine):
        k_t = kvb[s * 2 * cp:(s * 2 + 1) * cp].reshape(keys, head).T
        for h in (1, 0):
            for r in range(0, rows, ROWS):
                row0 = h * rows + r
                dq_t = dot_nn(k_t, get(ds_t.at[s], row0, ROWS))
                tab = get(tab_t, row0, ROWS)
                cos_q, sin_q = tab[:half_dim], tab[half_dim:]
                top, low = dq_t[:half_dim], dq_t[half_dim:]
                dq = jnp.concatenate([top * cos_q + low * sin_q, low * cos_q - top * sin_q], axis=0).astype(BF16).T
                out = get(o_t.at[s], row0, ROWS).T
                if h == 0:
                    dq_ref[core * mine + s, r:r + ROWS, :] = dq
                    o_ref[core * mine + s, r:r + ROWS, :] = out
                else:
                    dqsib[s, r:r + ROWS, :] = dq
                    osib[s, r:r + ROWS, :] = out
            if h == 1:
                out_copy(osib, o_ref, s).start()
                out_copy(dqsib, dq_ref, s).start()

    wait_bytes(qg, od_sem.at[0])
    wait_bytes(qg.at[0], od_sem.at[1])
    wait_by_chip(part, r_sem.at[0], lambda c: 2 * mine * (CORES * c + 1) + mine * (CORES * (chips - 1 - c) + 1) + 2)
    wait_by_chip(rbuf, r_sem.at[1], lambda c: 2 * mine * (CORES * (chips - 1 - c) + 1)
                 - (CORES * len(RELAYED) if c == 0 else 0))


def finish_kernel(o_in, dq_in, rbuf, tabs, o_hbm, dq_hbm, dk_hbm, dv_hbm, dk_buf, dv_buf, sem):
    copies = [pltpu.make_async_copy(o_in, o_hbm, sem.at[0]), pltpu.make_async_copy(dq_in, dq_hbm, sem.at[1]),
              pltpu.make_async_copy(dk_buf, dk_hbm, sem.at[2]), pltpu.make_async_copy(dv_buf, dv_hbm, sem.at[3])]
    for c in copies[:2]:
        c.start()
    head = tabs.shape[-1]
    scale = head ** -0.5
    cos_t, sin_t = tabs[0], tabs[1]
    seqs = dk_buf.shape[0]
    for b in range(seqs):
        dk = rbuf[2 * b]
        dv = rbuf[2 * b + 1]
        for c in range(2 * seqs, rbuf.shape[0], 2 * seqs):
            dk = dk + rbuf[c + 2 * b]
            dv = dv + rbuf[c + 2 * b + 1]
        dk = dk * scale
        dk_buf[b] = (dk * cos_t - pltpu.roll(dk, head // 2, 1) * sin_t).astype(BF16)
        dv_buf[b] = dv.astype(BF16)
    for c in copies[2:]:
        c.start()
    for c in copies:
        c.wait()


def solution(mesh):
    cp = mesh.shape["cp"]
    query_spec = P("dp", "cp", None, None)
    kv_spec = P("dp", "cp", None)
    pos_spec = P(("dp", "cp"))

    def per_device(query, key, value, positions, grad_out):
        seqs, blk, heads, head = query.shape
        rows = blk * heads
        chips = cp // CORES
        mine = seqs // CORES
        keys = cp * blk
        tiles = CORES * rows // LANES
        freq = np.power(float(ROPE_BASE), -2.0 * np.arange(head // 2) / head)
        freq = jnp.asarray(np.concatenate([freq, freq])[None, :].astype(np.float32))
        vmem = pl.BlockSpec(memory_space=pltpu.VMEM)
        hbm = pl.BlockSpec(memory_space=pltpu.HBM)
        dma = pltpu.SemaphoreType.DMA
        big = jax.ShapeDtypeStruct((seqs, rows, head), BF16)
        small = jax.ShapeDtypeStruct((seqs, blk, head), BF16)
        o_mid, dq_mid, rbuf, tabs = pl.pallas_call(
            functools.partial(attend_kernel, cp, blk),
            out_shape=[big, big, jax.ShapeDtypeStruct((chips * seqs * 2, blk, head), F32),
                       jax.ShapeDtypeStruct((2, blk, head), F32)],
            in_specs=[hbm] * 6,
            out_specs=[vmem, vmem, vmem, vmem],
            scratch_shapes=[
                pltpu.VMEM((2, seqs, blk, head), BF16),
                pltpu.VMEM((1, blk), jnp.int32),
                pltpu.VMEM((1, head), F32),
                pltpu.VMEM((2, mine, CORES, rows, head), BF16),
                pltpu.VMEM((mine, CORES * rows, head), BF16),
                pltpu.VMEM((CORES, 2, blk, head), F32),
                pltpu.VMEM((seqs, 2, blk, head), BF16),
                pltpu.VMEM((mine * 2 * cp, blk, head), BF16),
                pltpu.VMEM((mine, tiles, head, LANES), BF16),
                pltpu.VMEM((tiles, head, LANES), F32),
                pltpu.VMEM((tiles, blk, LANES), jnp.int32),
                pltpu.VMEM((tiles, 2 * CORES * blk, LANES), F32),
                pltpu.VMEM((1, CORES * rows), F32),
                pltpu.VMEM((tiles, keys, LANES), BF16),
                pltpu.VMEM((tiles, keys, LANES), F32),
                pltpu.VMEM((1, CORES * rows), F32),
                pltpu.VMEM((tiles, keys, LANES), BF16),
                pltpu.VMEM((mine, tiles, keys, LANES), BF16),
                pltpu.VMEM((mine, tiles, head, LANES), BF16),
                pltpu.VMEM((mine * 2 * cp, blk, head), F32),
                pltpu.VMEM((CORES * len(RELAYED), blk, head), F32),
                pltpu.VMEM((mine, rows, head), BF16),
                pltpu.VMEM((mine, rows, head), BF16),
                dma((3,)), dma, dma((mine,)), dma, dma((mine, 2)), dma, dma((2,)), dma, dma((2,)),
            ],
            compiler_params=pltpu.CompilerParams(collective_id=0, has_side_effects=True,
                                                 vmem_limit_bytes=32 * 2 ** 20),
            name="attend",
        )(*(pltpu.with_memory_space_constraint(a, pltpu.HBM) for a in (
            query.reshape(seqs, rows, head), grad_out.reshape(seqs, rows, head), key, value,
            positions.reshape(1, blk), freq)))
        attn, dquery, dkey, dvalue = pl.pallas_call(
            finish_kernel,
            out_shape=[big, big, small, small],
            in_specs=[vmem] * 4,
            out_specs=[hbm] * 4,
            scratch_shapes=[pltpu.VMEM((seqs, blk, head), BF16), pltpu.VMEM((seqs, blk, head), BF16), dma((4,))],
            compiler_params=pltpu.CompilerParams(vmem_limit_bytes=16 * 2 ** 20),
            name="finish",
        )(o_mid, dq_mid, rbuf, tabs)
        shape = (seqs, blk, heads, head)
        return attn.reshape(shape), dquery.reshape(shape), dkey, dvalue

    return jax.shard_map(per_device, mesh=mesh, in_specs=(query_spec, kv_spec, kv_spec, pos_spec, query_spec),
                         out_specs=(query_spec, query_spec, kv_spec, kv_spec), check_vma=False)
```
